32 devices in a mesh: row: 4 (over x, core), col: 8 (over z, y).
Axes of the slice: x: 2, y: 2, z: 4, core: 2. Of those that a mesh axis runs over, the one named last changes fastest.
Arguments:
- panel_rows: float32 [4096, 4096], P('row', 'col'), may hold values from -0.75 to 0.75
- owner_slot: int32 [8, 8], replicated, may hold values from -1 to 15, as said below
Outputs:
- packed: float32 [4, 16, 512, 512], P('row', 'col')
The draws below stay inside these ranges and needn't reach their ends.
Inputs may be any that keep to these rules, and one draw needn't show every extreme that they name: For j <= i, owner_slot[i, j] is the position of tile (i, j) among the 16 positions of group i // 2; tiles of one group have distinct positions; entries above the diagonal are -1. Position p lies on the device of col index p // 2.
All inputs are finite; a program needn't handle non-finite values.
Results may differ from the reference program's by a relative error of at most 0.0003.
Values sent between devices are 32-bit elements; how exact they have to be, the bound alone decides.
A program may use at most 128 MiB of HBM per device.

```python
import jax
import jax.numpy as jnp
from jax import lax

BLOCK = 512
K = 4096
ORDER = 4096
BR = 2
NB = 8
POS = 16
N_ROW = 4


def draw_owner_slot(key, part):
    groups = NB // BR
    block_row = jnp.arange(NB, dtype=jnp.int32)[:, None]
    block_col = jnp.arange(NB, dtype=jnp.int32)[None, :]
    row_keys = jax.random.split(jax.random.fold_in(key, 11), groups)
    orders = jax.vmap(lambda sub_key: jax.random.permutation(sub_key, POS))(row_keys).astype(jnp.int32)
    group_ids = jnp.arange(groups, dtype=jnp.int32)
    first_rows = group_ids * BR
    tile_total = BR * first_rows + BR * (BR + 1) // 2
    picked = jax.random.randint(jax.random.fold_in(key, 12), (groups,), 0, tile_total).astype(jnp.int32)
    top_place = jnp.argmax(orders == POS - 1, axis=1).astype(jnp.int32)
    offsets = top_place - picked
    row_group = block_row // BR
    first_own = row_group * BR
    index_in = (block_row * (block_row + 1) - first_own * (first_own + 1)) // 2 + block_col
    taken = (index_in + offsets[row_group[:, 0]][:, None]) % POS
    order_rows = orders[row_group[:, 0]]
    placed = jnp.take_along_axis(order_rows, taken, axis=1)
    return jnp.where(block_col <= block_row, placed, -1).astype(jnp.int32)


def levels(stream_key, extent, cuts, low, largest):
    level, own = 1.0, jax.random.fold_in(stream_key, 6)
    for dim, parts in cuts:
        draws = jnp.exp(jax.random.uniform(jax.random.fold_in(own, dim), (parts,), jnp.float32, low / len(cuts), largest / len(cuts)))
        level = level * jnp.repeat(draws, extent[dim] // parts).reshape([-1 if axis == dim else 1 for axis in range(len(extent))])
    return level


def noise(own_key, extent, width, bound, cuts=(), held_as=jnp.bfloat16):
    result = width * jax.random.normal(own_key, extent, jnp.float32)
    if cuts:
        result = result * levels(own_key, extent, cuts, -0.22, 0.18)
    return jnp.clip(result, -bound, bound).astype(held_as)


def setup_inputs(seed: int = 0) -> dict:
    key_list = jax.random.split(jax.random.key(seed), 3)
    return {
        "panel_rows": noise(key_list[0], (ORDER, K), (K ** -0.25), 0.75, ((0, 4), (1, 8)), jnp.float32),
        "owner_slot": draw_owner_slot(jax.random.fold_in(key_list[2], 71), 0),
    }


def slot_table(owner_slot, group_id, positions, per_group):
    blocks = owner_slot.shape[0]
    block_row = jnp.arange(blocks, dtype=jnp.int32)[:, None]
    block_col = jnp.arange(blocks, dtype=jnp.int32)[None, :]
    inside = (block_row // per_group == group_id) & (block_col <= block_row)
    wanted = jnp.arange(positions, dtype=jnp.int32)[:, None, None]
    matched = inside[None] & (owner_slot[None] == wanted)
    is_live = jnp.any(matched, axis=(1, 2))
    left_block = jnp.sum(jnp.where(matched, block_row[None], 0), axis=(1, 2)).astype(jnp.int32)
    right_block = jnp.sum(jnp.where(matched, block_col[None], 0), axis=(1, 2)).astype(jnp.int32)
    return left_block, right_block, is_live


def reference(panel_rows, owner_slot):
    tiles_all = panel_rows.reshape(NB, BLOCK, K)

    def group_tiles(group_id):
        left_block, right_block, is_live = slot_table(owner_slot, group_id, POS, BR)

        def single(packed_item):
            left_one, right_one, flag = packed_item

            def compute():
                return lax.dot_general(tiles_all[left_one], tiles_all[right_one], (((1,), (1,)), ((), ())),
                                       precision=lax.Precision.HIGHEST, preferred_element_type=jnp.float32)

            def blank():
                return jnp.zeros((BLOCK, BLOCK), jnp.float32)

            return lax.cond(flag, compute, blank)

        return lax.map(single, (left_block, right_block, is_live))

    return lax.map(group_tiles, jnp.arange(N_ROW, dtype=jnp.int32))
```

```python
import functools

import jax
import jax.numpy as jnp
from jax import lax
from jax.experimental import pallas as pl
from jax.experimental.pallas import tpu as pltpu
from jax.sharding import PartitionSpec as P

BLOCK = 512
EDGES = (0, 128, 256, 384, 512)
MESH = pl.DeviceIdType.MESH
NT = (((1,), (1,)), ((), ()))


def slot_table(owner_slot, group_id, positions, per_group):
    blocks = owner_slot.shape[0]
    block_row = jnp.arange(blocks, dtype=jnp.int32)[:, None]
    block_col = jnp.arange(blocks, dtype=jnp.int32)[None, :]
    inside = (block_row // per_group == group_id) & (block_col <= block_row)
    wanted = jnp.arange(positions, dtype=jnp.int32)[:, None, None]
    matched = inside[None] & (owner_slot[None] == wanted)
    is_live = jnp.any(matched, axis=(1, 2))
    left_block = jnp.sum(jnp.where(matched, block_row[None], 0), axis=(1, 2))
    right_block = jnp.sum(jnp.where(matched, block_col[None], 0), axis=(1, 2))
    return (left_block, right_block, is_live)


STAGES = len(EDGES) - 1
PIECES = []
for stage in range(STAGES):
    PIECES.append((stage, EDGES[stage], EDGES[stage + 1], 0, EDGES[stage + 1]))
    if stage:
        PIECES.append((stage, 0, EDGES[stage], EDGES[stage], EDGES[stage + 1]))


def kernel(rows_n, cols_n, per_group, slots, table, panel, out, *scratch):
    count = len(PIECES)
    scratch = list(scratch)

    def take(number):
        taken = scratch[:number]
        del scratch[:number]
        return taken

    held = take(STAGES)
    ysend, yrecv, zsend, zrecv = take(count), take(count), take(count), take(count)
    right_hi, right_lo, local_sem, load_recv, load_send, y_send, y_recv, z_send, z_recv = scratch
    row, col = lax.axis_index("row"), lax.axis_index("col")
    chips = rows_n // 2
    far = cols_n // 4
    x, core = row // 2, row % 2
    h, low, y = col // 4, (col // 2) % 2, col % 2
    sibling = (row + 1 - 2 * core, col)
    pair = (row, h * 4 + (1 - low) * 2 + y)
    across = (row, h * 4 + low * 2 + 1 - y)
    beside = [(((x + d) % chips) * 2 + core, col) for d in range(1, chips)]
    ahead = [(row, ((h + d) % far) * 4 + low * 2 + y) for d in range(1, far)]
    partners = [sibling, pair, across] + beside + ahead

    fetches = []
    for stage in range(STAGES):
        fetch = pltpu.make_async_copy(
            panel.at[:, pl.ds(EDGES[stage], EDGES[stage + 1] - EDGES[stage])],
            held[stage].at[pl.ds(row * per_group, per_group), low],
            local_sem.at[stage],
        )
        fetch.start()
        fetches.append(fetch)
    barrier = pltpu.get_barrier_semaphore()
    for device in partners:
        pl.semaphore_signal(barrier, inc=1, device_id=device, device_id_type=MESH)
    pl.semaphore_wait(barrier, len(partners))

    sent = []

    def push(stage, group, side, half, device):
        block = group * per_group + half
        copy = pltpu.make_async_remote_copy(
            src_ref=held[stage].at[block, side],
            dst_ref=held[stage].at[block, side],
            send_sem=load_send.at[len(sent)],
            recv_sem=load_recv.at[stage, block, side],
            device_id=device,
            device_id_type=MESH,
        )
        copy.start()
        sent.append(copy)

    def arrive(stage, group, side, half):
        block = group * per_group + half
        pltpu.make_async_remote_copy(
            src_ref=held[stage].at[block, side],
            dst_ref=held[stage].at[block, side],
            send_sem=load_send.at[0],
            recv_sem=load_recv.at[stage, block, side],
            device_id=sibling,
            device_id_type=MESH,
        ).wait_recv()

    cut = per_group // 2
    ups, downs = list(range(cut)), list(range(cut, per_group))
    others = [((x + chips - d) % chips) * 2 + core for d in range(1, chips)]

    def first(stage):
        fetches[stage].wait()
        for half in ups + downs:
            for device in beside:
                push(stage, row, low, half, device)
        for half in downs + ups:
            push(stage, row, low, half, pair)
        for half in ups + downs:
            push(stage, row, low, half, sibling)

    def second(stage):
        for group in others:
            for half in ups:
                arrive(stage, group, low, half)
                push(stage, group, low, half, pair)
                push(stage, group, low, half, sibling)
        for half in downs:
            arrive(stage, row, 1 - low, half)
            for device in beside:
                push(stage, row, 1 - low, half, device)
            push(stage, row, 1 - low, half, sibling)

    def third(stage):
        for group in others:
            for half in downs:
                arrive(stage, group, low, half)
                push(stage, group, low, half, sibling)
        for half in ups:
            arrive(stage, row, 1 - low, half)
            push(stage, row, 1 - low, half, sibling)
        for group in others:
            for half in ups + downs:
                arrive(stage, group, 1 - low, half)
                push(stage, group, 1 - low, half, sibling)
        for d in range(chips):
            group = ((x + d) % chips) * 2 + 1 - core
            for side in range(2):
                for half in range(per_group):
                    arrive(stage, group, side, half)

    depth = held[0].shape[-1]

    def split(value):
        top = value.astype(jnp.bfloat16)
        return top, (value - top.astype(jnp.float32)).astype(jnp.bfloat16)

    def strips(stage, position, emit, fresh=0):
        left, right = table[0, position], table[1, position]
        for part in range(fresh, stage + 1):
            for side in range(2):
                where = (slice(EDGES[part], EDGES[part + 1]), slice(side * depth, (side + 1) * depth))
                right_hi[where], right_lo[where] = split(held[part][right, side])

        def product(part, begin, end):
            total = None
            for side in range(2):
                span = slice(side * depth, (side + 1) * depth)
                top, rest = split(held[part][left, side])
                for one, two in ((rest, right_hi), (top, right_lo), (top, right_hi)):
                    term = lax.dot_general(one, two[begin:end, span], NT, preferred_element_type=jnp.float32)
                    total = term if total is None else total + term
            return total

        for number, (own_stage, r0, r1, c0, c1) in enumerate(PIECES):
            if own_stage == stage:
                for part in range(STAGES):
                    if r0 <= EDGES[part] < r1:
                        emit(number, EDGES[part] - r0, EDGES[part + 1] - r0, product(part, c0, c1))

    def numbers(stage):
        return [number for number, piece in enumerate(PIECES) if piece[0] == stage]

    def place(d, side_y, slot):
        return (((h + d) % far) * 4 + low * 2 + side_y) * slots + slot

    def y_copy(number, index):
        return pltpu.make_async_remote_copy(
            src_ref=ysend[number].at[index],
            dst_ref=yrecv[number].at[index],
            send_sem=y_send.at[number, index],
            recv_sem=y_recv.at[number, index],
            device_id=across,
            device_id_type=MESH,
        )

    def z_copy(number, index):
        return pltpu.make_async_remote_copy(
            src_ref=zsend[number].at[index],
            dst_ref=zrecv[number].at[index],
            send_sem=z_send.at[number, index],
            recv_sem=z_recv.at[number, index],
            device_id=(row, ((h + index // slots + 1) % far) * 4 + low * 2 + y),
            device_id_type=MESH,
        )

    tiles, hops = far * slots, (far - 1) * slots

    def y_work(stage):
        @pl.loop(0, tiles)
        def _(index):
            def emit(number, begin, end, value):
                ysend[number][index, begin:end, :] = value

            strips(stage, place(index // slots + 1, 1 - y, index % slots), emit)
            for number in numbers(stage):
                y_copy(number, index).start()

    def z_work(stage):
        @pl.loop(0, hops)
        def _(index):
            def emit(number, begin, end, value):
                zsend[number][index, begin:end, :] = value

            strips(stage, place(index // slots + 1, y, index % slots), emit)
            for number in numbers(stage):
                y_copy(number, index).wait_recv()
                zsend[number][index] += yrecv[number][index]
                z_copy(number, index).start()

    first(0)
    for stage in range(STAGES):
        second(stage)
        if stage + 1 < STAGES:
            first(stage + 1)
        if stage:
            z_work(stage - 1)
        third(stage)
        y_work(stage)
    z_work(STAGES - 1)

    @pl.loop(0, slots)
    def _(slot):
        def emit(number, begin, end, value):
            _, r0, _, c0, c1 = PIECES[number]
            out[slot, r0 + begin:r0 + end, c0:c1] = value

        for stage in range(STAGES):
            strips(stage, place(0, y, slot), emit, stage)
        for number, (_, r0, r1, c0, c1) in enumerate(PIECES):
            y_copy(number, hops + slot).wait_recv()
            out[slot, r0:r1, c0:c1] += yrecv[number][hops + slot]

    for number, (_, r0, r1, c0, c1) in enumerate(PIECES):
        @pl.loop(0, hops)
        def _(index):
            z_copy(number, index).wait_recv()
            slot = index % slots
            out[slot, r0:r1, c0:c1] += zrecv[number][index]

    for slot in range(slots):
        live = table[2, place(0, y, slot)]
        out[slot] = jnp.where(live > 0, out[slot], 0.0)

    for copy in sent:
        copy.wait_send()
    for number in range(count):
        @pl.loop(0, tiles)
        def _(index):
            y_copy(number, index).wait_send()

        @pl.loop(0, hops)
        def _(index):
            z_copy(number, index).wait_send()


def general(panel_rows, owner_slot):
    rows_n = lax.axis_size("row")
    cols_n = lax.axis_size("col")
    slab_rows, depth = panel_rows.shape
    per_group = slab_rows // BLOCK
    blocks = per_group * rows_n
    row_tiles = per_group * (blocks - per_group) + per_group * (per_group + 1) // 2
    slots = (row_tiles + cols_n - 1) // cols_n
    positions = cols_n * slots
    table = jnp.stack([part.astype(jnp.int32) for part in slot_table(owner_slot, lax.axis_index("row"), positions, per_group)])
    chips, far = rows_n // 2, cols_n // 4
    pushes = per_group * ((chips - 1) * 4 + 3) + per_group * (chips - 1)
    tiles = far * slots
    hops = (far - 1) * slots
    summed = pl.pallas_call(
        functools.partial(kernel, rows_n, cols_n, per_group, slots),
        out_shape=jax.ShapeDtypeStruct((slots, BLOCK, BLOCK), jnp.float32),
        in_specs=[pl.BlockSpec(memory_space=pltpu.SMEM), pl.BlockSpec(memory_space=pl.ANY)],
        out_specs=pl.BlockSpec(memory_space=pltpu.VMEM),
        scratch_shapes=[pltpu.VMEM((blocks, 2, EDGES[stage + 1] - EDGES[stage], depth), jnp.float32) for stage in range(STAGES)]
        + [
            pltpu.VMEM((number, r1 - r0, c1 - c0), jnp.float32)
            for number in (tiles, tiles, hops, hops)
            for _, r0, r1, c0, c1 in PIECES
        ]
        + [
            pltpu.VMEM((BLOCK, 2 * depth), jnp.bfloat16),
            pltpu.VMEM((BLOCK, 2 * depth), jnp.bfloat16),
            pltpu.SemaphoreType.DMA((STAGES,)),
            pltpu.SemaphoreType.DMA((STAGES, blocks, 2)),
            pltpu.SemaphoreType.DMA((STAGES * pushes,)),
            pltpu.SemaphoreType.DMA((len(PIECES), tiles)),
            pltpu.SemaphoreType.DMA((len(PIECES), tiles)),
            pltpu.SemaphoreType.DMA((len(PIECES), hops)),
            pltpu.SemaphoreType.DMA((len(PIECES), hops)),
        ],
        compiler_params=pltpu.CompilerParams(
            collective_id=0, has_side_effects=True, vmem_limit_bytes=60 * 2**20
        ),
        cost_estimate=pl.CostEstimate(flops=2 * positions * BLOCK * BLOCK * depth, bytes_accessed=2**22, transcendentals=0),
    )(table, panel_rows.reshape(per_group, BLOCK, depth))
    return summed[None]


STRIPS = 8
WIDE = 4
FAR, ACROSS, PASS, OWN = range(4)


def fast_pieces():
    width, lanes = BLOCK // STRIPS, BLOCK // WIDE
    pieces = []
    for stage in range(STRIPS):
        reach = min(lanes * (stage + 1), BLOCK)
        pieces.append((stage, width * stage, width * (stage + 1), 0, reach))
        if 0 < stage < WIDE:
            pieces.append((stage, 0, width * stage, reach - lanes, reach))
    return pieces


FAST_PIECES = fast_pieces()


def fast_kernel(slots, owner, panel, out, *scratch):
    count = len(FAST_PIECES)
    scratch = list(scratch)

    def take(number):
        taken = scratch[:number]
        del scratch[:number]
        return taken

    ysend, yrecv, zsend, zrecv = take(count), take(count), take(count), take(count)
    held, high, rest, total, table, local_sem, load_recv, load_send, y_send, y_recv, z_send, z_recv = scratch
    per_group = panel.shape[0]
    depth = panel.shape[-1]
    width, lanes = BLOCK // STRIPS, BLOCK // WIDE
    row, col = lax.axis_index("row"), lax.axis_index("col")
    x, core = row // 2, row % 2
    h, low, y = col // 4, (col // 2) % 2, col % 2
    sibling = (row + 1 - 2 * core, col)
    pair = (row, h * 4 + (1 - low) * 2 + y)
    across = (row, h * 4 + low * 2 + 1 - y)
    opposite = (row, (1 - h) * 4 + (1 - low) * 2 + y)
    beside = ((1 - x) * 2 + core, col)
    partners = [sibling, pair, across, opposite, beside]
    halves = range(per_group)

    fetches = []
    for strip in range(STRIPS):
        fetch = pltpu.make_async_copy(
            panel.at[:, pl.ds(strip * width, width)],
            held.at[pl.ds(row * per_group, per_group), low, pl.ds(strip * width, width)],
            local_sem.at[strip],
        )
        fetch.start()
        fetches.append(fetch)
    barrier = pltpu.get_barrier_semaphore()
    for device in partners:
        pl.semaphore_signal(barrier, inc=1, device_id=device, device_id_type=MESH)
    pl.semaphore_wait(barrier, len(partners))

    always, first_x, second_x = [], [], []

    def load_copy(number, strip, group, half, side, device):
        block = group * per_group + half
        where = held.at[block, side, pl.ds(strip * width, width)]
        return pltpu.make_async_remote_copy(
            src_ref=where,
            dst_ref=where,
            send_sem=load_send.at[number],
            recv_sem=load_recv.at[strip, block, side],
            device_id=device,
            device_id_type=MESH,
        )

    def push(strip, group, half, side, device, log):
        entry = (len(always) + len(first_x) + len(second_x), strip, group, half, side, device)
        load_copy(*entry).start()
        log.append(entry)

    def arrive(strip, group, half, side):
        load_copy(0, strip, group, half, side, sibling).wait_recv()

    def ahead(strip):
        @pl.when(x == 0)
        def _():
            for half in halves:
                push(strip, row, half, low, beside, first_x)

    def begin(strip):
        fetches[strip].wait()
        if strip == 0:
            ahead(0)
        for half in halves:
            push(strip, row, half, low, pair, always)
        for half in halves:
            push(strip, row, half, low, sibling, always)

    other, flip = x * 2 + 1 - core, 1 - low

    def gather(stage):
        strips = (2 * stage, 2 * stage + 1) if stage < WIDE else ()
        for strip in strips:
            for half in halves:
                arrive(strip, row, half, flip)

                @pl.when(x == 0)
                def _():
                    push(strip, row, half, flip, beside, first_x)

                push(strip, row, half, flip, sibling, always)
            if strip + 1 < STRIPS:
                ahead(strip + 1)

        @pl.when(x == 1)
        def _():
            for side in (low, flip):
                for half in halves:
                    arrive(stage, core, half, side)
                    push(stage, core, half, side, sibling, second_x)

        for strip in strips:
            for side in range(2):
                for half in halves:
                    arrive(strip, other, half, side)

        @pl.when(x == 1)
        def _():
            for side in range(2):
                for half in halves:
                    arrive(stage, 1 - core, half, side)

    def split(block, begin_row, rows):
        for side in range(2):
            value = held[block, side, begin_row:begin_row + rows, :]
            top = value.astype(jnp.bfloat16)
            span = slice(side * depth, (side + 1) * depth)
            high[block, begin_row:begin_row + rows, span] = top
            rest[block, begin_row:begin_row + rows, span] = (value - top.astype(jnp.float32)).astype(jnp.bfloat16)

    def convert(stage):
        @pl.loop(0, per_group)
        def _(half):
            if stage < WIDE:
                split(row * per_group + half, lanes * stage, lanes)
            split(other * per_group + half, width * stage, width)

        @pl.when(x == 1)
        def _():
            @pl.loop(0, 2 * per_group)
            def _(block):
                split(block, width * stage, width)

    for kind, place in (
        (FAR, (1 - h) * 4 + (1 - low) * 2 + 1 - y),
        (ACROSS, h * 4 + low * 2 + 1 - y),
        (PASS, (1 - h) * 4 + (1 - low) * 2 + y),
        (OWN, h * 4 + low * 2 + y),
    ):
        for slot in range(slots):
            position = place * slots + slot
            left, right, live = row * per_group, row * per_group, 0
            for half in halves:
                for block in range(owner.shape[1]):
                    hit = owner[row * per_group + half, block] == position
                    left = jnp.where(hit, row * per_group + half, left)
                    right = jnp.where(hit, block, right)
                    live = jnp.where(hit, 1, live)
            table[0, kind * slots + slot] = left
            table[1, kind * slots + slot] = right
            table[2, kind * slots + slot] = live

    def numbers(stage):
        return [number for number, piece in enumerate(FAST_PIECES) if piece[0] == stage]

    def product(number, entry):
        _, r0, r1, c0, c1 = FAST_PIECES[number]
        wide, tall = table[0, entry], table[1, entry]
        top, low_part = high[tall, r0:r1, :], rest[tall, r0:r1, :]
        both = lax.dot_general(
            jnp.concatenate([top, low_part], axis=0), high[wide, c0:c1, :], NT, preferred_element_type=jnp.float32
        )
        cross = lax.dot_general(top, rest[wide, c0:c1, :], NT, preferred_element_type=jnp.float32)
        return both[r1 - r0:] + cross + both[:r1 - r0]

    def y_copy(number, index):
        return pltpu.make_async_remote_copy(
            src_ref=ysend[number].at[index],
            dst_ref=yrecv[number].at[index],
            send_sem=y_send.at[number, index],
            recv_sem=y_recv.at[number, index],
            device_id=across,
            device_id_type=MESH,
        )

    def z_copy(number, index):
        return pltpu.make_async_remote_copy(
            src_ref=zsend[number].at[index],
            dst_ref=zrecv[number].at[index],
            send_sem=z_send.at[number, index],
            recv_sem=z_recv.at[number, index],
            device_id=opposite,
            device_id_type=MESH,
        )

    def y_work(stage, kind):
        @pl.loop(0, slots)
        def _(slot):
            index = kind * slots + slot
            for number in numbers(stage):
                ysend[number][index] = product(number, index)
                y_copy(number, index).start()

    def z_work(stage):
        @pl.loop(0, slots)
        def _(slot):
            for number in numbers(stage):
                value = product(number, PASS * slots + slot)
                y_copy(number, FAR * slots + slot).wait_recv()
                zsend[number][slot] = value + yrecv[number][FAR * slots + slot]
                z_copy(number, slot).start()

    def own_work(stage):
        @pl.loop(0, slots)
        def _(slot):
            for number in numbers(stage):
                _, r0, r1, c0, c1 = FAST_PIECES[number]
                total[slot, r0:r1, c0:c1] = product(number, OWN * slots + slot)

    def collect(stage):
        for number in numbers(stage):
            _, r0, r1, c0, c1 = FAST_PIECES[number]

            @pl.loop(0, slots)
            def _(slot):
                y_copy(number, ACROSS * slots + slot).wait_recv()
                z_copy(number, slot).wait_recv()
                total[slot, r0:r1, c0:c1] += yrecv[number][ACROSS * slots + slot] + zrecv[number][slot]

    def finish(part):
        for slot in range(slots):
            live = table[2, OWN * slots + slot]
            for c0 in range(0, BLOCK, lanes):
                value = total[slot, part * lanes:(part + 1) * lanes, c0:c0 + lanes].T
                out[slot, c0:c0 + lanes, part * lanes:(part + 1) * lanes] = jnp.where(live > 0, value, 0.0)

    for strip in range(4):
        begin(strip)
    for stage in range(STRIPS):
        gather(stage)
        for strip in (2 * stage + 4, 2 * stage + 5):
            if strip < STRIPS:
                begin(strip)
        convert(stage)
        y_work(stage, FAR)
        y_work(stage, ACROSS)
        own_work(stage)
        z_work(stage)
    for stage in range(STRIPS):
        collect(stage)
        if stage >= WIDE - 1 and stage % 2:
            for part in ((0, 1) if stage == WIDE - 1 else (stage // 2,)):
                finish(part)

    for entry in always:
        load_copy(*entry).wait_send()

    @pl.when(x == 0)
    def _():
        for entry in first_x:
            load_copy(*entry).wait_send()

    @pl.when(x == 1)
    def _():
        for entry in second_x:
            load_copy(*entry).wait_send()

    for number in range(count):
        @pl.loop(0, 2 * slots)
        def _(index):
            y_copy(number, index).wait_send()

        @pl.loop(0, slots)
        def _(index):
            z_copy(number, index).wait_send()


def quick(panel_rows, owner_slot):
    rows_n = lax.axis_size("row")
    cols_n = lax.axis_size("col")
    slab_rows, depth = panel_rows.shape
    per_group = slab_rows // BLOCK
    blocks = per_group * rows_n
    row_tiles = per_group * (blocks - per_group) + per_group * (per_group + 1) // 2
    slots = (row_tiles + cols_n - 1) // cols_n
    positions = cols_n * slots
    count = len(FAST_PIECES)
    pushes = STRIPS * per_group * 7
    summed = pl.pallas_call(
        functools.partial(fast_kernel, slots),
        out_shape=jax.ShapeDtypeStruct((slots, BLOCK, BLOCK), jnp.float32),
        in_specs=[pl.BlockSpec(memory_space=pltpu.SMEM), pl.BlockSpec(memory_space=pl.ANY)],
        out_specs=pl.BlockSpec(memory_space=pltpu.VMEM),
        scratch_shapes=[
            pltpu.VMEM((number, r1 - r0, c1 - c0), jnp.float32)
            for number in (2 * slots, 2 * slots, slots, slots)
            for _, r0, r1, c0, c1 in FAST_PIECES
        ]
        + [
            pltpu.VMEM((blocks, 2, BLOCK, depth), jnp.float32),
            pltpu.VMEM((blocks, BLOCK, 2 * depth), jnp.bfloat16),
            pltpu.VMEM((blocks, BLOCK, 2 * depth), jnp.bfloat16),
            pltpu.VMEM((slots, BLOCK, BLOCK), jnp.float32),
            pltpu.SMEM((3, 4 * slots), jnp.int32),
            pltpu.SemaphoreType.DMA((STRIPS,)),
            pltpu.SemaphoreType.DMA((STRIPS, blocks, 2)),
            pltpu.SemaphoreType.DMA((pushes,)),
            pltpu.SemaphoreType.DMA((count, 2 * slots)),
            pltpu.SemaphoreType.DMA((count, 2 * slots)),
            pltpu.SemaphoreType.DMA((count, slots)),
            pltpu.SemaphoreType.DMA((count, slots)),
        ],
        compiler_params=pltpu.CompilerParams(
            collective_id=0, has_side_effects=True, vmem_limit_bytes=60 * 2**20
        ),
        cost_estimate=pl.CostEstimate(flops=2 * positions * BLOCK * BLOCK * depth, bytes_accessed=2**22, transcendentals=0),
    )(owner_slot, panel_rows.reshape(per_group, BLOCK, depth))
    return summed[None]


def body(panel_rows, owner_slot):
    if lax.axis_size("row") == 4 and lax.axis_size("col") == 8:
        return quick(panel_rows, owner_slot)
    return general(panel_rows, owner_slot)


def solution(mesh):
    placed = (P("row", "col"), P())
    return jax.shard_map(
        body, mesh=mesh, in_specs=placed, out_specs=P("row", "col", None, None), check_vma=False
    )
```

```python
import functools

import jax
import jax.numpy as jnp
from jax import lax
from jax.experimental import pallas as pl
from jax.experimental.pallas import tpu as pltpu
from jax.sharding import PartitionSpec as P

BLOCK = 512
EDGES = (0, 128, 256, 384, 512)
MESH = pl.DeviceIdType.MESH
NT = (((1,), (1,)), ((), ()))


def slot_table(owner_slot, group_id, positions, per_group):
    blocks = owner_slot.shape[0]
    block_row = jnp.arange(blocks, dtype=jnp.int32)[:, None]
    block_col = jnp.arange(blocks, dtype=jnp.int32)[None, :]
    inside = (block_row // per_group == group_id) & (block_col <= block_row)
    wanted = jnp.arange(positions, dtype=jnp.int32)[:, None, None]
    matched = inside[None] & (owner_slot[None] == wanted)
    is_live = jnp.any(matched, axis=(1, 2))
    left_block = jnp.sum(jnp.where(matched, block_row[None], 0), axis=(1, 2))
    right_block = jnp.sum(jnp.where(matched, block_col[None], 0), axis=(1, 2))
    return (left_block, right_block, is_live)


STAGES = len(EDGES) - 1
PIECES = []
for stage in range(STAGES):
    PIECES.append((stage, EDGES[stage], EDGES[stage + 1], 0, EDGES[stage + 1]))
    if stage:
        PIECES.append((stage, 0, EDGES[stage], EDGES[stage], EDGES[stage + 1]))


def kernel(rows_n, cols_n, per_group, slots, table, panel, out, *scratch):
    count = len(PIECES)
    scratch = list(scratch)

    def take(number):
        taken = scratch[:number]
        del scratch[:number]
        return taken

    held = take(STAGES)
    ysend, yrecv, zsend, zrecv = take(count), take(count), take(count), take(count)
    right_hi, right_lo, local_sem, load_recv, load_send, y_send, y_recv, z_send, z_recv = scratch
    row, col = lax.axis_index("row"), lax.axis_index("col")
    chips = rows_n // 2
    far = cols_n // 4
    x, core = row // 2, row % 2
    h, low, y = col // 4, (col // 2) % 2, col % 2
    sibling = (row + 1 - 2 * core, col)
    pair = (row, h * 4 + (1 - low) * 2 + y)
    across = (row, h * 4 + low * 2 + 1 - y)
    beside = [(((x + d) % chips) * 2 + core, col) for d in range(1, chips)]
    ahead = [(row, ((h + d) % far) * 4 + low * 2 + y) for d in range(1, far)]
    partners = [sibling, pair, across] + beside + ahead

    fetches = []
    for stage in range(STAGES):
        fetch = pltpu.make_async_copy(
            panel.at[:, pl.ds(EDGES[stage], EDGES[stage + 1] - EDGES[stage])],
            held[stage].at[pl.ds(row * per_group, per_group), low],
            local_sem.at[stage],
        )
        fetch.start()
        fetches.append(fetch)
    barrier = pltpu.get_barrier_semaphore()
    for device in partners:
        pl.semaphore_signal(barrier, inc=1, device_id=device, device_id_type=MESH)
    pl.semaphore_wait(barrier, len(partners))

    sent = []

    def push(stage, group, side, half, device):
        block = group * per_group + half
        copy = pltpu.make_async_remote_copy(
            src_ref=held[stage].at[block, side],
            dst_ref=held[stage].at[block, side],
            send_sem=load_send.at[len(sent)],
            recv_sem=load_recv.at[stage, block, side],
            device_id=device,
            device_id_type=MESH,
        )
        copy.start()
        sent.append(copy)

    def arrive(stage, group, side, half):
        block = group * per_group + half
        pltpu.make_async_remote_copy(
            src_ref=held[stage].at[block, side],
            dst_ref=held[stage].at[block, side],
            send_sem=load_send.at[0],
            recv_sem=load_recv.at[stage, block, side],
            device_id=sibling,
            device_id_type=MESH,
        ).wait_recv()

    cut = per_group // 2
    ups, downs = list(range(cut)), list(range(cut, per_group))
    others = [((x + chips - d) % chips) * 2 + core for d in range(1, chips)]

    def first(stage):
        fetches[stage].wait()
        for half in ups + downs:
            for device in beside:
                push(stage, row, low, half, device)
        for half in downs + ups:
            push(stage, row, low, half, pair)
        for half in ups + downs:
            push(stage, row, low, half, sibling)

    def second(stage):
        for group in others:
            for half in ups:
                arrive(stage, group, low, half)
                push(stage, group, low, half, pair)
                push(stage, group, low, half, sibling)
        for half in downs:
            arrive(stage, row, 1 - low, half)
            for device in beside:
                push(stage, row, 1 - low, half, device)
            push(stage, row, 1 - low, half, sibling)

    def third(stage):
        for group in others:
            for half in downs:
                arrive(stage, group, low, half)
                push(stage, group, low, half, sibling)
        for half in ups:
            arrive(stage, row, 1 - low, half)
            push(stage, row, 1 - low, half, sibling)
        for group in others:
            for half in ups + downs:
                arrive(stage, group, 1 - low, half)
                push(stage, group, 1 - low, half, sibling)
        for d in range(chips):
            group = ((x + d) % chips) * 2 + 1 - core
            for side in range(2):
                for half in range(per_group):
                    arrive(stage, group, side, half)

    depth = held[0].shape[-1]

    def split(value):
        top = value.astype(jnp.bfloat16)
        return top, (value - top.astype(jnp.float32)).astype(jnp.bfloat16)

    def strips(stage, position, emit, fresh=0):
        left, right = table[0, position], table[1, position]
        for part in range(fresh, stage + 1):
            for side in range(2):
                where = (slice(EDGES[part], EDGES[part + 1]), slice(side * depth, (side + 1) * depth))
                right_hi[where], right_lo[where] = split(held[part][right, side])

        def product(part, begin, end):
            total = None
            for side in range(2):
                span = slice(side * depth, (side + 1) * depth)
                top, rest = split(held[part][left, side])
                for one, two in ((rest, right_hi), (top, right_lo), (top, right_hi)):
                    term = lax.dot_general(one, two[begin:end, span], NT, preferred_element_type=jnp.float32)
                    total = term if total is None else total + term
            return total

        for number, (own_stage, r0, r1, c0, c1) in enumerate(PIECES):
            if own_stage == stage:
                for part in range(STAGES):
                    if r0 <= EDGES[part] < r1:
                        emit(number, EDGES[part] - r0, EDGES[part + 1] - r0, product(part, c0, c1))

    def numbers(stage):
        return [number for number, piece in enumerate(PIECES) if piece[0] == stage]

    def place(d, side_y, slot):
        return (((h + d) % far) * 4 + low * 2 + side_y) * slots + slot

    def y_copy(number, index):
        return pltpu.make_async_remote_copy(
            src_ref=ysend[number].at[index],
            dst_ref=yrecv[number].at[index],
            send_sem=y_send.at[number, index],
            recv_sem=y_recv.at[number, index],
            device_id=across,
            device_id_type=MESH,
        )

    def z_copy(number, index):
        return pltpu.make_async_remote_copy(
            src_ref=zsend[number].at[index],
            dst_ref=zrecv[number].at[index],
            send_sem=z_send.at[number, index],
            recv_sem=z_recv.at[number, index],
            device_id=(row, ((h + index // slots + 1) % far) * 4 + low * 2 + y),
            device_id_type=MESH,
        )

    tiles, hops = far * slots, (far - 1) * slots

    def y_work(stage):
        @pl.loop(0, tiles)
        def _(index):
            def emit(number, begin, end, value):
                ysend[number][index, begin:end, :] = value

            strips(stage, place(index // slots + 1, 1 - y, index % slots), emit)
            for number in numbers(stage):
                y_copy(number, index).start()

    def z_work(stage):
        @pl.loop(0, hops)
        def _(index):
            def emit(number, begin, end, value):
                zsend[number][index, begin:end, :] = value

            strips(stage, place(index // slots + 1, y, index % slots), emit)
            for number in numbers(stage):
                y_copy(number, index).wait_recv()
                zsend[number][index] += yrecv[number][index]
                z_copy(number, index).start()

    first(0)
    for stage in range(STAGES):
        second(stage)
        if stage + 1 < STAGES:
            first(stage + 1)
        if stage:
            z_work(stage - 1)
        third(stage)
        y_work(stage)
    z_work(STAGES - 1)

    @pl.loop(0, slots)
    def _(slot):
        def emit(number, begin, end, value):
            _, r0, _, c0, c1 = PIECES[number]
            out[slot, r0 + begin:r0 + end, c0:c1] = value

        for stage in range(STAGES):
            strips(stage, place(0, y, slot), emit, stage)
        for number, (_, r0, r1, c0, c1) in enumerate(PIECES):
            y_copy(number, hops + slot).wait_recv()
            out[slot, r0:r1, c0:c1] += yrecv[number][hops + slot]

    for number, (_, r0, r1, c0, c1) in enumerate(PIECES):
        @pl.loop(0, hops)
        def _(index):
            z_copy(number, index).wait_recv()
            slot = index % slots
            out[slot, r0:r1, c0:c1] += zrecv[number][index]

    for slot in range(slots):
        live = table[2, place(0, y, slot)]
        out[slot] = jnp.where(live > 0, out[slot], 0.0)

    for copy in sent:
        copy.wait_send()
    for number in range(count):
        @pl.loop(0, tiles)
        def _(index):
            y_copy(number, index).wait_send()

        @pl.loop(0, hops)
        def _(index):
            z_copy(number, index).wait_send()


def general(panel_rows, owner_slot):
    rows_n = lax.axis_size("row")
    cols_n = lax.axis_size("col")
    slab_rows, depth = panel_rows.shape
    per_group = slab_rows // BLOCK
    blocks = per_group * rows_n
    row_tiles = per_group * (blocks - per_group) + per_group * (per_group + 1) // 2
    slots = (row_tiles + cols_n - 1) // cols_n
    positions = cols_n * slots
    table = jnp.stack([part.astype(jnp.int32) for part in slot_table(owner_slot, lax.axis_index("row"), positions, per_group)])
    chips, far = rows_n // 2, cols_n // 4
    pushes = per_group * ((chips - 1) * 4 + 3) + per_group * (chips - 1)
    tiles = far * slots
    hops = (far - 1) * slots
    summed = pl.pallas_call(
        functools.partial(kernel, rows_n, cols_n, per_group, slots),
        out_shape=jax.ShapeDtypeStruct((slots, BLOCK, BLOCK), jnp.float32),
        in_specs=[pl.BlockSpec(memory_space=pltpu.SMEM), pl.BlockSpec(memory_space=pl.ANY)],
        out_specs=pl.BlockSpec(memory_space=pltpu.VMEM),
        scratch_shapes=[pltpu.VMEM((blocks, 2, EDGES[stage + 1] - EDGES[stage], depth), jnp.float32) for stage in range(STAGES)]
        + [
            pltpu.VMEM((number, r1 - r0, c1 - c0), jnp.float32)
            for number in (tiles, tiles, hops, hops)
            for _, r0, r1, c0, c1 in PIECES
        ]
        + [
            pltpu.VMEM((BLOCK, 2 * depth), jnp.bfloat16),
            pltpu.VMEM((BLOCK, 2 * depth), jnp.bfloat16),
            pltpu.SemaphoreType.DMA((STAGES,)),
            pltpu.SemaphoreType.DMA((STAGES, blocks, 2)),
            pltpu.SemaphoreType.DMA((STAGES * pushes,)),
            pltpu.SemaphoreType.DMA((len(PIECES), tiles)),
            pltpu.SemaphoreType.DMA((len(PIECES), tiles)),
            pltpu.SemaphoreType.DMA((len(PIECES), hops)),
            pltpu.SemaphoreType.DMA((len(PIECES), hops)),
        ],
        compiler_params=pltpu.CompilerParams(
            collective_id=0, has_side_effects=True, vmem_limit_bytes=60 * 2**20
        ),
        cost_estimate=pl.CostEstimate(flops=2 * positions * BLOCK * BLOCK * depth, bytes_accessed=2**22, transcendentals=0),
    )(table, panel_rows.reshape(per_group, BLOCK, depth))
    return summed[None]


LANES = 128
TALL = (0, 64, 128, 192, 256, 320, 384, 448, 512)
REACH = (128, 256, 384, 512, 512, 512, 512, 512)
STEP = 64
STEPS = BLOCK // STEP
AREAS = ((3, 0, 128), (3, 128, 256), (5, 256, 384), (7, 384, 512))
FULL = REACH.index(BLOCK)
FAST_STAGES = len(REACH)
FIRST = 4
PLAN = ((0, 0), (1, 0), (2, 0), (4, 4), (4, 5), (0, 1), (1, 1), (2, 1), (4, 6), (4, 7), (0, 2), (1, 2), (2, 2), (0, 3), (1, 3), (2, 3), (0, 4), (0, 5), (2, 4), (1, 4), (3, 3), (0, 6), (2, 5), (1, 5), (3, 5), (0, 7), (2, 6), (1, 6), (1, 7), (2, 7), (3, 7))
HELD = ()
FAR, ACROSS, PASS, OWN = range(4)


def fast_pieces():
    pieces, before = [], 0
    for stage, reach in enumerate(REACH):
        pieces.append((stage, TALL[stage], TALL[stage + 1], 0, reach))
        if stage and reach > before:
            pieces.append((stage, 0, TALL[stage], before, reach))
        before = reach
    return pieces


FAST_PIECES = fast_pieces()


def fast_kernel(slots, owner, panel, out, *scratch):
    count = len(FAST_PIECES)
    scratch = list(scratch)

    def take(number):
        taken = scratch[:number]
        del scratch[:number]
        return taken

    ysend, yrecv, zsend, zrecv = take(count), take(count), take(count), take(count)
    held, high, rest, total, done, table, local_sem, load_recv, cross_recv, load_send, y_send, f_recv, o_recv, z_send, z_recv, out_sem = scratch
    per_group = panel.shape[0]
    depth = panel.shape[-1]
    row, col = lax.axis_index("row"), lax.axis_index("col")
    x, core = row // 2, row % 2
    h, low, y = col // 4, (col // 2) % 2, col % 2
    sibling = (row + 1 - 2 * core, col)
    pair = (row, h * 4 + (1 - low) * 2 + y)
    across = (row, h * 4 + low * 2 + 1 - y)
    opposite = (row, (1 - h) * 4 + (1 - low) * 2 + y)
    beside = ((1 - x) * 2 + core, col)
    partners = [sibling, pair, across, opposite, beside]
    halves = range(per_group)

    fetches = []
    for step in range(STEPS):
        fetch = pltpu.make_async_copy(
            panel.at[:, pl.ds(step * STEP, STEP)],
            held.at[pl.ds(row * per_group, per_group), low, pl.ds(step * STEP, STEP)],
            local_sem.at[step],
        )
        fetch.start()
        fetches.append(fetch)
    barrier = pltpu.get_barrier_semaphore()
    for device in partners:
        pl.semaphore_signal(barrier, inc=1, device_id=device, device_id_type=MESH)
    pl.semaphore_wait(barrier, len(partners))

    def load_copy(arrivals, step, group, side, device, kind):
        rows = pl.ds(0, BLOCK) if step is None else pl.ds(step * STEP, STEP)
        where = held.at[pl.ds(group * per_group, per_group), side, rows]
        return pltpu.make_async_remote_copy(
            src_ref=where,
            dst_ref=where,
            send_sem=load_send.at[kind],
            recv_sem=arrivals.at[0 if step is None else step, group % 2, side],
            device_id=device,
            device_id_type=MESH,
        )

    def push(arrivals, step, group, side, device, kind):
        load_copy(arrivals, step, group, side, device, kind).start()

    def arrive(arrivals, step, group, side):
        load_copy(arrivals, step, group, side, sibling, 0).wait_recv()

    other, flip = x * 2 + 1 - core, 1 - low

    def forward(step, side, kind):
        @pl.when(x == 0)
        def _():
            push(cross_recv, step, row, side, beside, kind)

    def begin(step):
        fetches[step].wait()
        if step == 0:
            forward(0, low, 3)
        push(load_recv, step, row, low, pair, 0)
        push(load_recv, step, row, low, sibling, 1)

    def gather(stage):
        start = REACH[stage - 1] if stage else 0
        steps = range(start // STEP, REACH[stage] // STEP)
        parts = range(TALL[stage] // STEP, TALL[stage + 1] // STEP)
        for step in steps:
            arrive(load_recv, step, row, flip)
            forward(step, flip, 4)
            if step + 1 < STEPS:
                forward(step + 1, low, 3)
            push(load_recv, step, row, flip, sibling, 2)

        @pl.when(x == 1)
        def _():
            for part in parts:
                for kind, side in ((5, low), (6, flip)):
                    arrive(cross_recv, part, core, side)
                    push(cross_recv, part, core, side, sibling, kind)

        for step in steps:
            for side in range(2):
                arrive(load_recv, step, other, side)

        @pl.when(x == 1)
        def _():
            for part in parts:
                for side in range(2):
                    arrive(cross_recv, part, 1 - core, side)

    def split(block, begin_row, end_row):
        for side in range(2):
            value = held[block, side, begin_row:end_row, :]
            top = value.astype(jnp.bfloat16)
            span = slice(side * depth, (side + 1) * depth)
            high[block, begin_row:end_row, span] = top
            rest[block, begin_row:end_row, span] = (value - top.astype(jnp.float32)).astype(jnp.bfloat16)

    def convert(stage):
        start = REACH[stage - 1] if stage else 0

        @pl.loop(0, per_group)
        def _(half):
            if start < REACH[stage]:
                split(row * per_group + half, start, REACH[stage])
            split(other * per_group + half, TALL[stage], TALL[stage + 1])

        @pl.when(x == 1)
        def _():
            @pl.loop(0, 2 * per_group)
            def _(block):
                split(block, TALL[stage], TALL[stage + 1])

    def numbers(stage):
        return [number for number, piece in enumerate(FAST_PIECES) if piece[0] == stage]

    def product(area, entry):
        r0, r1, c0, c1 = area
        wide, tall = table[0, entry], table[1, entry]
        top, low_part = high[tall, r0:r1, :], rest[tall, r0:r1, :]
        both = lax.dot_general(
            jnp.concatenate([top, low_part], axis=0), high[wide, c0:c1, :], NT, preferred_element_type=jnp.float32
        )
        cross = lax.dot_general(top, rest[wide, c0:c1, :], NT, preferred_element_type=jnp.float32)
        return both[r1 - r0:] + cross + both[:r1 - r0]

    def y_copy(number, kind, index):
        return pltpu.make_async_remote_copy(
            src_ref=ysend[number].at[index],
            dst_ref=yrecv[number].at[index],
            send_sem=y_send,
            recv_sem=(f_recv.at[number, index] if kind == FAR else o_recv.at[number]),
            device_id=across,
            device_id_type=MESH,
        )

    def z_copy(number, index):
        return pltpu.make_async_remote_copy(
            src_ref=zsend[number].at[index],
            dst_ref=zrecv[number].at[index],
            send_sem=z_send,
            recv_sem=z_recv.at[number],
            device_id=opposite,
            device_id_type=MESH,
        )

    def y_work(stage, kind):
        @pl.loop(0, slots)
        def _(slot):
            index = kind * slots + slot
            for number in numbers(stage):
                ysend[number][index] = product(FAST_PIECES[number][1:], index)
                y_copy(number, kind, index).start()

    def z_work(stage):
        @pl.loop(0, slots)
        def _(slot):
            for number in numbers(stage):
                value = product(FAST_PIECES[number][1:], PASS * slots + slot)
                y_copy(number, FAR, FAR * slots + slot).wait_recv()
                zsend[number][slot] = value + yrecv[number][FAR * slots + slot]
                if stage in HELD:
                    @pl.when(h != low)
                    def _():
                        z_copy(number, slot).start()
                else:
                    z_copy(number, slot).start()

    def release(stage):
        @pl.when(h == low)
        def _():
            for number in numbers(stage):
                @pl.loop(0, slots)
                def _(slot):
                    z_copy(number, slot).start()

    def own_work(stage):
        @pl.loop(0, slots)
        def _(slot):
            for last, r0, r1 in AREAS:
                if last == stage:
                    total[slot, r0:r1, :] = product((r0, r1, 0, BLOCK), OWN * slots + slot)

    def collect(stage):
        for number in numbers(stage):
            _, r0, r1, c0, c1 = FAST_PIECES[number]
            y_copy(number, ACROSS, pl.ds(ACROSS * slots, slots)).wait_recv()
            z_copy(number, pl.ds(0, slots)).wait_recv()

            @pl.loop(0, slots)
            def _(slot):
                total[slot, r0:r1, c0:c1] += yrecv[number][ACROSS * slots + slot] + zrecv[number][slot]

    def store(part, slot):
        span = pl.ds(part * LANES, LANES)
        return pltpu.make_async_copy(done.at[slot, :, span], out.at[slot, :, span], out_sem.at[part, slot])

    def finish(part):
        for slot in range(slots):
            live = table[2, OWN * slots + slot]
            for c0 in range(0, BLOCK, LANES):
                value = total[slot, part * LANES:(part + 1) * LANES, c0:c0 + LANES].T
                done[slot, c0:c0 + LANES, part * LANES:(part + 1) * LANES] = jnp.where(live > 0, value, 0.0)
            store(part, slot).start()

    for step in range(FIRST):
        begin(step)
    for kind, place in (
        (FAR, (1 - h) * 4 + (1 - low) * 2 + 1 - y),
        (ACROSS, h * 4 + low * 2 + 1 - y),
        (PASS, (1 - h) * 4 + (1 - low) * 2 + y),
        (OWN, h * 4 + low * 2 + y),
    ):
        for slot in range(slots):
            position = place * slots + slot
            left, right, live = row * per_group, row * per_group, 0
            for half in halves:
                for block in range(owner.shape[1]):
                    hit = owner[row * per_group + half, block] == position
                    left = jnp.where(hit, row * per_group + half, left)
                    right = jnp.where(hit, block, right)
                    live = jnp.where(hit, 1, live)
            table[0, kind * slots + slot] = left
            table[1, kind * slots + slot] = right
            table[2, kind * slots + slot] = live

    def supply(stage):
        gather(stage)
        convert(stage)
        y_work(stage, FAR)

    def relay(stage):
        y_work(stage, ACROSS)

    acts = (supply, relay, z_work, own_work, begin, release)
    for act, argument in PLAN:
        acts[act](argument)
    ready = 0
    for stage in range(FAST_STAGES):
        collect(stage)
        while stage >= FULL and (ready + 1) * LANES <= TALL[stage + 1]:
            finish(ready)
            ready += 1

    for side, kind in ((low, 0), (low, 1), (flip, 2)):
        load_copy(load_recv, None, row, side, sibling, kind).wait_send()

    @pl.when(x == 0)
    def _():
        for side, kind in ((low, 3), (flip, 4)):
            load_copy(cross_recv, None, row, side, sibling, kind).wait_send()

    @pl.when(x == 1)
    def _():
        for side, kind in ((low, 5), (flip, 6)):
            load_copy(cross_recv, None, core, side, sibling, kind).wait_send()

    for area, sem in ((held.at[pl.ds(0, slots)], y_send), (held.at[pl.ds(0, slots), 0], z_send)):
        pltpu.make_async_remote_copy(
            src_ref=area, dst_ref=area, send_sem=sem, recv_sem=o_recv.at[0], device_id=across, device_id_type=MESH
        ).wait_send()

    for part in range(BLOCK // LANES):
        for slot in range(slots):
            store(part, slot).wait()


def quick(panel_rows, owner_slot):
    rows_n = lax.axis_size("row")
    cols_n = lax.axis_size("col")
    slab_rows, depth = panel_rows.shape
    per_group = slab_rows // BLOCK
    blocks = per_group * rows_n
    row_tiles = per_group * (blocks - per_group) + per_group * (per_group + 1) // 2
    slots = (row_tiles + cols_n - 1) // cols_n
    positions = cols_n * slots
    count = len(FAST_PIECES)
    summed = pl.pallas_call(
        functools.partial(fast_kernel, slots),
        out_shape=jax.ShapeDtypeStruct((slots, BLOCK, BLOCK), jnp.float32),
        in_specs=[pl.BlockSpec(memory_space=pltpu.SMEM), pl.BlockSpec(memory_space=pl.ANY)],
        out_specs=pl.BlockSpec(memory_space=pl.ANY),
        scratch_shapes=[
            pltpu.VMEM((number, r1 - r0, c1 - c0), jnp.float32)
            for number in (2 * slots, 2 * slots, slots, slots)
            for _, r0, r1, c0, c1 in FAST_PIECES
        ]
        + [
            pltpu.VMEM((blocks, 2, BLOCK, depth), jnp.float32),
            pltpu.VMEM((blocks, BLOCK, 2 * depth), jnp.bfloat16),
            pltpu.VMEM((blocks, BLOCK, 2 * depth), jnp.bfloat16),
            pltpu.VMEM((slots, BLOCK, BLOCK), jnp.float32),
            pltpu.VMEM((slots, BLOCK, BLOCK), jnp.float32),
            pltpu.SMEM((3, 4 * slots), jnp.int32),
            pltpu.SemaphoreType.DMA((STEPS,)),
            pltpu.SemaphoreType.DMA((STEPS, 2, 2)),
            pltpu.SemaphoreType.DMA((STEPS, 2, 2)),
            pltpu.SemaphoreType.DMA((7,)),
            pltpu.SemaphoreType.DMA(()),
            pltpu.SemaphoreType.DMA((count, slots)),
            pltpu.SemaphoreType.DMA((count,)),
            pltpu.SemaphoreType.DMA(()),
            pltpu.SemaphoreType.DMA((count,)),
            pltpu.SemaphoreType.DMA((BLOCK // LANES, slots)),
        ],
        compiler_params=pltpu.CompilerParams(
            collective_id=0, has_side_effects=True, vmem_limit_bytes=60 * 2**20
        ),
        cost_estimate=pl.CostEstimate(flops=2 * positions * BLOCK * BLOCK * depth, bytes_accessed=2**22, transcendentals=0),
    )(owner_slot, panel_rows.reshape(per_group, BLOCK, depth))
    return summed[None]


def body(panel_rows, owner_slot):
    if lax.axis_size("row") == 4 and lax.axis_size("col") == 8:
        return quick(panel_rows, owner_slot)
    return general(panel_rows, owner_slot)


def solution(mesh):
    placed = (P("row", "col"), P())
    return jax.shard_map(
        body, mesh=mesh, in_specs=placed, out_specs=P("row", "col", None, None), check_vma=False
    )
```

```python
import functools

import jax
import jax.numpy as jnp
from jax import lax
from jax.experimental import pallas as pl
from jax.experimental.pallas import tpu as pltpu
from jax.sharding import PartitionSpec as P

BLOCK = 512
EDGES = (0, 128, 256, 384, 512)
MESH = pl.DeviceIdType.MESH
NT = (((1,), (1,)), ((), ()))


def slot_table(owner_slot, group_id, positions, per_group):
    blocks = owner_slot.shape[0]
    block_row = jnp.arange(blocks, dtype=jnp.int32)[:, None]
    block_col = jnp.arange(blocks, dtype=jnp.int32)[None, :]
    inside = (block_row // per_group == group_id) & (block_col <= block_row)
    wanted = jnp.arange(positions, dtype=jnp.int32)[:, None, None]
    matched = inside[None] & (owner_slot[None] == wanted)
    is_live = jnp.any(matched, axis=(1, 2))
    left_block = jnp.sum(jnp.where(matched, block_row[None], 0), axis=(1, 2))
    right_block = jnp.sum(jnp.where(matched, block_col[None], 0), axis=(1, 2))
    return (left_block, right_block, is_live)


STAGES = len(EDGES) - 1
PIECES = []
for stage in range(STAGES):
    PIECES.append((stage, EDGES[stage], EDGES[stage + 1], 0, EDGES[stage + 1]))
    if stage:
        PIECES.append((stage, 0, EDGES[stage], EDGES[stage], EDGES[stage + 1]))


def kernel(rows_n, cols_n, per_group, slots, table, panel, out, *scratch):
    count = len(PIECES)
    scratch = list(scratch)

    def take(number):
        taken = scratch[:number]
        del scratch[:number]
        return taken

    held = take(STAGES)
    ysend, yrecv, zsend, zrecv = take(count), take(count), take(count), take(count)
    right_hi, right_lo, local_sem, load_recv, load_send, y_send, y_recv, z_send, z_recv = scratch
    row, col = lax.axis_index("row"), lax.axis_index("col")
    chips = rows_n // 2
    far = cols_n // 4
    x, core = row // 2, row % 2
    h, low, y = col // 4, (col // 2) % 2, col % 2
    sibling = (row + 1 - 2 * core, col)
    pair = (row, h * 4 + (1 - low) * 2 + y)
    across = (row, h * 4 + low * 2 + 1 - y)
    beside = [(((x + d) % chips) * 2 + core, col) for d in range(1, chips)]
    ahead = [(row, ((h + d) % far) * 4 + low * 2 + y) for d in range(1, far)]
    partners = [sibling, pair, across] + beside + ahead

    fetches = []
    for stage in range(STAGES):
        fetch = pltpu.make_async_copy(
            panel.at[:, pl.ds(EDGES[stage], EDGES[stage + 1] - EDGES[stage])],
            held[stage].at[pl.ds(row * per_group, per_group), low],
            local_sem.at[stage],
        )
        fetch.start()
        fetches.append(fetch)
    barrier = pltpu.get_barrier_semaphore()
    for device in partners:
        pl.semaphore_signal(barrier, inc=1, device_id=device, device_id_type=MESH)
    pl.semaphore_wait(barrier, len(partners))

    sent = []

    def push(stage, group, side, half, device):
        block = group * per_group + half
        copy = pltpu.make_async_remote_copy(
            src_ref=held[stage].at[block, side],
            dst_ref=held[stage].at[block, side],
            send_sem=load_send.at[len(sent)],
            recv_sem=load_recv.at[stage, block, side],
            device_id=device,
            device_id_type=MESH,
        )
        copy.start()
        sent.append(copy)

    def arrive(stage, group, side, half):
        block = group * per_group + half
        pltpu.make_async_remote_copy(
            src_ref=held[stage].at[block, side],
            dst_ref=held[stage].at[block, side],
            send_sem=load_send.at[0],
            recv_sem=load_recv.at[stage, block, side],
            device_id=sibling,
            device_id_type=MESH,
        ).wait_recv()

    cut = per_group // 2
    ups, downs = list(range(cut)), list(range(cut, per_group))
    others = [((x + chips - d) % chips) * 2 + core for d in range(1, chips)]

    def first(stage):
        fetches[stage].wait()
        for half in ups + downs:
            for device in beside:
                push(stage, row, low, half, device)
        for half in downs + ups:
            push(stage, row, low, half, pair)
        for half in ups + downs:
            push(stage, row, low, half, sibling)

    def second(stage):
        for group in others:
            for half in ups:
                arrive(stage, group, low, half)
                push(stage, group, low, half, pair)
                push(stage, group, low, half, sibling)
        for half in downs:
            arrive(stage, row, 1 - low, half)
            for device in beside:
                push(stage, row, 1 - low, half, device)
            push(stage, row, 1 - low, half, sibling)

    def third(stage):
        for group in others:
            for half in downs:
                arrive(stage, group, low, half)
                push(stage, group, low, half, sibling)
        for half in ups:
            arrive(stage, row, 1 - low, half)
            push(stage, row, 1 - low, half, sibling)
        for group in others:
            for half in ups + downs:
                arrive(stage, group, 1 - low, half)
                push(stage, group, 1 - low, half, sibling)
        for d in range(chips):
            group = ((x + d) % chips) * 2 + 1 - core
            for side in range(2):
                for half in range(per_group):
                    arrive(stage, group, side, half)

    depth = held[0].shape[-1]

    def split(value):
        top = value.astype(jnp.bfloat16)
        return top, (value - top.astype(jnp.float32)).astype(jnp.bfloat16)

    def strips(stage, position, emit, fresh=0):
        left, right = table[0, position], table[1, position]
        for part in range(fresh, stage + 1):
            for side in range(2):
                where = (slice(EDGES[part], EDGES[part + 1]), slice(side * depth, (side + 1) * depth))
                right_hi[where], right_lo[where] = split(held[part][right, side])

        def product(part, begin, end):
            total = None
            for side in range(2):
                span = slice(side * depth, (side + 1) * depth)
                top, rest = split(held[part][left, side])
                for one, two in ((rest, right_hi), (top, right_lo), (top, right_hi)):
                    term = lax.dot_general(one, two[begin:end, span], NT, preferred_element_type=jnp.float32)
                    total = term if total is None else total + term
            return total

        for number, (own_stage, r0, r1, c0, c1) in enumerate(PIECES):
            if own_stage == stage:
                for part in range(STAGES):
                    if r0 <= EDGES[part] < r1:
                        emit(number, EDGES[part] - r0, EDGES[part + 1] - r0, product(part, c0, c1))

    def numbers(stage):
        return [number for number, piece in enumerate(PIECES) if piece[0] == stage]

    def place(d, side_y, slot):
        return (((h + d) % far) * 4 + low * 2 + side_y) * slots + slot

    def y_copy(number, index):
        return pltpu.make_async_remote_copy(
            src_ref=ysend[number].at[index],
            dst_ref=yrecv[number].at[index],
            send_sem=y_send.at[number, index],
            recv_sem=y_recv.at[number, index],
            device_id=across,
            device_id_type=MESH,
        )

    def z_copy(number, index):
        return pltpu.make_async_remote_copy(
            src_ref=zsend[number].at[index],
            dst_ref=zrecv[number].at[index],
            send_sem=z_send.at[number, index],
            recv_sem=z_recv.at[number, index],
            device_id=(row, ((h + index // slots + 1) % far) * 4 + low * 2 + y),
            device_id_type=MESH,
        )

    tiles, hops = far * slots, (far - 1) * slots

    def y_work(stage):
        @pl.loop(0, tiles)
        def _(index):
            def emit(number, begin, end, value):
                ysend[number][index, begin:end, :] = value

            strips(stage, place(index // slots + 1, 1 - y, index % slots), emit)
            for number in numbers(stage):
                y_copy(number, index).start()

    def z_work(stage):
        @pl.loop(0, hops)
        def _(index):
            def emit(number, begin, end, value):
                zsend[number][index, begin:end, :] = value

            strips(stage, place(index // slots + 1, y, index % slots), emit)
            for number in numbers(stage):
                y_copy(number, index).wait_recv()
                zsend[number][index] += yrecv[number][index]
                z_copy(number, index).start()

    first(0)
    for stage in range(STAGES):
        second(stage)
        if stage + 1 < STAGES:
            first(stage + 1)
        if stage:
            z_work(stage - 1)
        third(stage)
        y_work(stage)
    z_work(STAGES - 1)

    @pl.loop(0, slots)
    def _(slot):
        def emit(number, begin, end, value):
            _, r0, _, c0, c1 = PIECES[number]
            out[slot, r0 + begin:r0 + end, c0:c1] = value

        for stage in range(STAGES):
            strips(stage, place(0, y, slot), emit, stage)
        for number, (_, r0, r1, c0, c1) in enumerate(PIECES):
            y_copy(number, hops + slot).wait_recv()
            out[slot, r0:r1, c0:c1] += yrecv[number][hops + slot]

    for number, (_, r0, r1, c0, c1) in enumerate(PIECES):
        @pl.loop(0, hops)
        def _(index):
            z_copy(number, index).wait_recv()
            slot = index % slots
            out[slot, r0:r1, c0:c1] += zrecv[number][index]

    for slot in range(slots):
        live = table[2, place(0, y, slot)]
        out[slot] = jnp.where(live > 0, out[slot], 0.0)

    for copy in sent:
        copy.wait_send()
    for number in range(count):
        @pl.loop(0, tiles)
        def _(index):
            y_copy(number, index).wait_send()

        @pl.loop(0, hops)
        def _(index):
            z_copy(number, index).wait_send()


def general(panel_rows, owner_slot):
    rows_n = lax.axis_size("row")
    cols_n = lax.axis_size("col")
    slab_rows, depth = panel_rows.shape
    per_group = slab_rows // BLOCK
    blocks = per_group * rows_n
    row_tiles = per_group * (blocks - per_group) + per_group * (per_group + 1) // 2
    slots = (row_tiles + cols_n - 1) // cols_n
    positions = cols_n * slots
    table = jnp.stack([part.astype(jnp.int32) for part in slot_table(owner_slot, lax.axis_index("row"), positions, per_group)])
    chips, far = rows_n // 2, cols_n // 4
    pushes = per_group * ((chips - 1) * 4 + 3) + per_group * (chips - 1)
    tiles = far * slots
    hops = (far - 1) * slots
    summed = pl.pallas_call(
        functools.partial(kernel, rows_n, cols_n, per_group, slots),
        out_shape=jax.ShapeDtypeStruct((slots, BLOCK, BLOCK), jnp.float32),
        in_specs=[pl.BlockSpec(memory_space=pltpu.SMEM), pl.BlockSpec(memory_space=pl.ANY)],
        out_specs=pl.BlockSpec(memory_space=pltpu.VMEM),
        scratch_shapes=[pltpu.VMEM((blocks, 2, EDGES[stage + 1] - EDGES[stage], depth), jnp.float32) for stage in range(STAGES)]
        + [
            pltpu.VMEM((number, r1 - r0, c1 - c0), jnp.float32)
            for number in (tiles, tiles, hops, hops)
            for _, r0, r1, c0, c1 in PIECES
        ]
        + [
            pltpu.VMEM((BLOCK, 2 * depth), jnp.bfloat16),
            pltpu.VMEM((BLOCK, 2 * depth), jnp.bfloat16),
            pltpu.SemaphoreType.DMA((STAGES,)),
            pltpu.SemaphoreType.DMA((STAGES, blocks, 2)),
            pltpu.SemaphoreType.DMA((STAGES * pushes,)),
            pltpu.SemaphoreType.DMA((len(PIECES), tiles)),
            pltpu.SemaphoreType.DMA((len(PIECES), tiles)),
            pltpu.SemaphoreType.DMA((len(PIECES), hops)),
            pltpu.SemaphoreType.DMA((len(PIECES), hops)),
        ],
        compiler_params=pltpu.CompilerParams(
            collective_id=0, has_side_effects=True, vmem_limit_bytes=60 * 2**20
        ),
        cost_estimate=pl.CostEstimate(flops=2 * positions * BLOCK * BLOCK * depth, bytes_accessed=2**22, transcendentals=0),
    )(table, panel_rows.reshape(per_group, BLOCK, depth))
    return summed[None]


LANES = 128
TALL = (0, 64, 128, 192, 256, 320, 384, 448, 512)
REACH = (128, 256, 384, 512, 512, 512, 512, 512)
STEP = 64
STEPS = BLOCK // STEP
AREAS = ((3, 0, 128), (3, 128, 256), (5, 256, 384), (7, 384, 512))
FULL = REACH.index(BLOCK)
FAST_STAGES = len(REACH)
FIRST = 4
PLAN = ((0, 0), (1, 0), (2, 0), (4, 4), (4, 5), (0, 1), (1, 1), (2, 1), (4, 6), (4, 7), (0, 2), (1, 2), (2, 2), (0, 3), (1, 3), (2, 3), (0, 4), (0, 5), (2, 4), (1, 4), (3, 3), (0, 6), (2, 5), (1, 5), (3, 5), (0, 7), (2, 6), (1, 6), (1, 7), (2, 7), (3, 7))
HELD = ()
FAR, ACROSS, PASS, OWN = range(4)


def fast_pieces():
    pieces, before = [], 0
    for stage, reach in enumerate(REACH):
        pieces.append((stage, TALL[stage], TALL[stage + 1], 0, reach))
        if stage and reach > before:
            pieces.append((stage, 0, TALL[stage], before, reach))
        before = reach
    return pieces


FAST_PIECES = fast_pieces()


def fast_kernel(slots, owner, panel, out, *scratch):
    count = len(FAST_PIECES)
    scratch = list(scratch)

    def take(number):
        taken = scratch[:number]
        del scratch[:number]
        return taken

    ysend, yrecv, zsend, zrecv = take(count), take(count), take(count), take(count)
    held, high, rest, total, table, local_sem, load_recv, cross_recv, load_send, y_send, f_recv, o_recv, z_send, z_recv = scratch
    per_group = panel.shape[0]
    depth = panel.shape[-1]
    row, col = lax.axis_index("row"), lax.axis_index("col")
    x, core = row // 2, row % 2
    h, low, y = col // 4, (col // 2) % 2, col % 2
    sibling = (row + 1 - 2 * core, col)
    pair = (row, h * 4 + (1 - low) * 2 + y)
    across = (row, h * 4 + low * 2 + 1 - y)
    opposite = (row, (1 - h) * 4 + (1 - low) * 2 + y)
    beside = ((1 - x) * 2 + core, col)
    partners = [sibling, pair, across, opposite, beside]
    halves = range(per_group)

    fetches = []
    for step in range(STEPS):
        fetch = pltpu.make_async_copy(
            panel.at[:, pl.ds(step * STEP, STEP)],
            held.at[pl.ds(row * per_group, per_group), low, pl.ds(step * STEP, STEP)],
            local_sem.at[step],
        )
        fetch.start()
        fetches.append(fetch)
    barrier = pltpu.get_barrier_semaphore()
    for device in partners:
        pl.semaphore_signal(barrier, inc=1, device_id=device, device_id_type=MESH)
    pl.semaphore_wait(barrier, len(partners))

    def load_copy(arrivals, step, group, side, device, kind):
        rows = pl.ds(0, BLOCK) if step is None else pl.ds(step * STEP, STEP)
        where = held.at[pl.ds(group * per_group, per_group), side, rows]
        return pltpu.make_async_remote_copy(
            src_ref=where,
            dst_ref=where,
            send_sem=load_send.at[kind],
            recv_sem=arrivals.at[0 if step is None else step, group % 2, side],
            device_id=device,
            device_id_type=MESH,
        )

    def push(arrivals, step, group, side, device, kind):
        load_copy(arrivals, step, group, side, device, kind).start()

    def arrive(arrivals, step, group, side):
        load_copy(arrivals, step, group, side, sibling, 0).wait_recv()

    other, flip = x * 2 + 1 - core, 1 - low

    def forward(step, side, kind):
        @pl.when(x == 0)
        def _():
            push(cross_recv, step, row, side, beside, kind)

    def begin(step):
        fetches[step].wait()
        if step == 0:
            forward(0, low, 3)
        push(load_recv, step, row, low, pair, 0)
        push(load_recv, step, row, low, sibling, 1)

    def gather(stage):
        start = REACH[stage - 1] if stage else 0
        steps = range(start // STEP, REACH[stage] // STEP)
        parts = range(TALL[stage] // STEP, TALL[stage + 1] // STEP)
        for step in steps:
            arrive(load_recv, step, row, flip)
            forward(step, flip, 4)
            if step + 1 < STEPS:
                forward(step + 1, low, 3)
            push(load_recv, step, row, flip, sibling, 2)

        @pl.when(x == 1)
        def _():
            for part in parts:
                for kind, side in ((5, low), (6, flip)):
                    arrive(cross_recv, part, core, side)
                    push(cross_recv, part, core, side, sibling, kind)

        for step in steps:
            for side in range(2):
                arrive(load_recv, step, other, side)

        @pl.when(x == 1)
        def _():
            for part in parts:
                for side in range(2):
                    arrive(cross_recv, part, 1 - core, side)

    def split(block, begin_row, end_row):
        for side in range(2):
            value = held[block, side, begin_row:end_row, :]
            top = value.astype(jnp.bfloat16)
            span = slice(side * depth, (side + 1) * depth)
            high[block, begin_row:end_row, span] = top
            rest[block, begin_row:end_row, span] = (value - top.astype(jnp.float32)).astype(jnp.bfloat16)

    def convert(stage):
        start = REACH[stage - 1] if stage else 0

        @pl.loop(0, per_group)
        def _(half):
            if start < REACH[stage]:
                split(row * per_group + half, start, REACH[stage])
            split(other * per_group + half, TALL[stage], TALL[stage + 1])

        @pl.when(x == 1)
        def _():
            @pl.loop(0, 2 * per_group)
            def _(block):
                split(block, TALL[stage], TALL[stage + 1])

    def numbers(stage):
        return [number for number, piece in enumerate(FAST_PIECES) if piece[0] == stage]

    def product(area, entry):
        r0, r1, c0, c1 = area
        wide, tall = table[0, entry], table[1, entry]
        top, low_part = high[tall, r0:r1, :], rest[tall, r0:r1, :]
        both = lax.dot_general(
            jnp.concatenate([top, low_part], axis=0), high[wide, c0:c1, :], NT, preferred_element_type=jnp.float32
        )
        cross = lax.dot_general(top, rest[wide, c0:c1, :], NT, preferred_element_type=jnp.float32)
        return both[r1 - r0:] + cross + both[:r1 - r0]

    def y_copy(number, kind, index):
        return pltpu.make_async_remote_copy(
            src_ref=ysend[number].at[index],
            dst_ref=yrecv[number].at[index],
            send_sem=y_send,
            recv_sem=(f_recv.at[number, index] if kind == FAR else o_recv.at[number]),
            device_id=across,
            device_id_type=MESH,
        )

    def z_copy(number, index):
        return pltpu.make_async_remote_copy(
            src_ref=zsend[number].at[index],
            dst_ref=zrecv[number].at[index],
            send_sem=z_send,
            recv_sem=z_recv.at[number],
            device_id=opposite,
            device_id_type=MESH,
        )

    def y_work(stage, kind):
        @pl.loop(0, slots)
        def _(slot):
            index = kind * slots + slot
            for number in numbers(stage):
                ysend[number][index] = product(FAST_PIECES[number][1:], index)
                y_copy(number, kind, index).start()

    def z_work(stage):
        @pl.loop(0, slots)
        def _(slot):
            for number in numbers(stage):
                value = product(FAST_PIECES[number][1:], PASS * slots + slot)
                y_copy(number, FAR, FAR * slots + slot).wait_recv()
                zsend[number][slot] = value + yrecv[number][FAR * slots + slot]
                if stage in HELD:
                    @pl.when(h != low)
                    def _():
                        z_copy(number, slot).start()
                else:
                    z_copy(number, slot).start()

    def release(stage):
        @pl.when(h == low)
        def _():
            for number in numbers(stage):
                @pl.loop(0, slots)
                def _(slot):
                    z_copy(number, slot).start()

    def own_work(stage):
        @pl.loop(0, slots)
        def _(slot):
            for last, r0, r1 in AREAS:
                if last == stage:
                    total[slot, r0:r1, :] = product((r0, r1, 0, BLOCK), OWN * slots + slot)

    def collect(stage):
        for number in numbers(stage):
            _, r0, r1, c0, c1 = FAST_PIECES[number]
            y_copy(number, ACROSS, pl.ds(ACROSS * slots, slots)).wait_recv()
            z_copy(number, pl.ds(0, slots)).wait_recv()

            @pl.loop(0, slots)
            def _(slot):
                total[slot, r0:r1, c0:c1] += yrecv[number][ACROSS * slots + slot] + zrecv[number][slot]

    def finish(part):
        for slot in range(slots):
            live = table[2, OWN * slots + slot]
            for c0 in range(0, BLOCK, LANES):
                value = total[slot, part * LANES:(part + 1) * LANES, c0:c0 + LANES].T
                out[slot, c0:c0 + LANES, part * LANES:(part + 1) * LANES] = jnp.where(live > 0, value, 0.0)

    for step in range(FIRST):
        begin(step)
    for kind, place in (
        (FAR, (1 - h) * 4 + (1 - low) * 2 + 1 - y),
        (ACROSS, h * 4 + low * 2 + 1 - y),
        (PASS, (1 - h) * 4 + (1 - low) * 2 + y),
        (OWN, h * 4 + low * 2 + y),
    ):
        for slot in range(slots):
            position = place * slots + slot
            left, right, live = row * per_group, row * per_group, 0
            for half in halves:
                for block in range(owner.shape[1]):
                    hit = owner[row * per_group + half, block] == position
                    left = jnp.where(hit, row * per_group + half, left)
                    right = jnp.where(hit, block, right)
                    live = jnp.where(hit, 1, live)
            table[0, kind * slots + slot] = left
            table[1, kind * slots + slot] = right
            table[2, kind * slots + slot] = live

    def supply(stage):
        gather(stage)
        convert(stage)
        y_work(stage, FAR)

    def relay(stage):
        y_work(stage, ACROSS)

    acts = (supply, relay, z_work, own_work, begin, release)
    for act, argument in PLAN:
        acts[act](argument)
    ready = 0
    for stage in range(FAST_STAGES):
        collect(stage)
        while stage >= FULL and (ready + 1) * LANES <= TALL[stage + 1]:
            finish(ready)
            ready += 1

    for side, kind in ((low, 0), (low, 1), (flip, 2)):
        load_copy(load_recv, None, row, side, sibling, kind).wait_send()

    @pl.when(x == 0)
    def _():
        for side, kind in ((low, 3), (flip, 4)):
            load_copy(cross_recv, None, row, side, sibling, kind).wait_send()

    @pl.when(x == 1)
    def _():
        for side, kind in ((low, 5), (flip, 6)):
            load_copy(cross_recv, None, core, side, sibling, kind).wait_send()

    for area, sem in ((held.at[pl.ds(0, slots)], y_send), (held.at[pl.ds(0, slots), 0], z_send)):
        pltpu.make_async_remote_copy(
            src_ref=area, dst_ref=area, send_sem=sem, recv_sem=o_recv.at[0], device_id=across, device_id_type=MESH
        ).wait_send()


def quick(panel_rows, owner_slot):
    rows_n = lax.axis_size("row")
    cols_n = lax.axis_size("col")
    slab_rows, depth = panel_rows.shape
    per_group = slab_rows // BLOCK
    blocks = per_group * rows_n
    row_tiles = per_group * (blocks - per_group) + per_group * (per_group + 1) // 2
    slots = (row_tiles + cols_n - 1) // cols_n
    positions = cols_n * slots
    count = len(FAST_PIECES)
    summed = pl.pallas_call(
        functools.partial(fast_kernel, slots),
        out_shape=pltpu.VMEM((slots, BLOCK, BLOCK), jnp.float32),
        in_specs=[pl.BlockSpec(memory_space=pltpu.SMEM), pl.BlockSpec(memory_space=pl.ANY)],
        out_specs=pl.BlockSpec(memory_space=pltpu.VMEM),
        scratch_shapes=[
            pltpu.VMEM((number, r1 - r0, c1 - c0), jnp.float32)
            for number in (2 * slots, 2 * slots, slots, slots)
            for _, r0, r1, c0, c1 in FAST_PIECES
        ]
        + [
            pltpu.VMEM((blocks, 2, BLOCK, depth), jnp.float32),
            pltpu.VMEM((blocks, BLOCK, 2 * depth), jnp.bfloat16),
            pltpu.VMEM((blocks, BLOCK, 2 * depth), jnp.bfloat16),
            pltpu.VMEM((slots, BLOCK, BLOCK), jnp.float32),
            pltpu.SMEM((3, 4 * slots), jnp.int32),
            pltpu.SemaphoreType.DMA((STEPS,)),
            pltpu.SemaphoreType.DMA((STEPS, 2, 2)),
            pltpu.SemaphoreType.DMA((STEPS, 2, 2)),
            pltpu.SemaphoreType.DMA((7,)),
            pltpu.SemaphoreType.DMA(()),
            pltpu.SemaphoreType.DMA((count, slots)),
            pltpu.SemaphoreType.DMA((count,)),
            pltpu.SemaphoreType.DMA(()),
            pltpu.SemaphoreType.DMA((count,)),
        ],
        compiler_params=pltpu.CompilerParams(
            collective_id=0, has_side_effects=True, vmem_limit_bytes=54 * 2**20
        ),
        cost_estimate=pl.CostEstimate(flops=2 * positions * BLOCK * BLOCK * depth, bytes_accessed=2**22, transcendentals=0),
    )(owner_slot, panel_rows.reshape(per_group, BLOCK, depth))
    return summed[None]


def body(panel_rows, owner_slot):
    if lax.axis_size("row") == 4 and lax.axis_size("col") == 8:
        return quick(panel_rows, owner_slot)
    return general(panel_rows, owner_slot)


def solution(mesh):
    placed = (P("row", "col"), P())
    return jax.shard_map(
        body, mesh=mesh, in_specs=placed, out_specs=P("row", "col", None, None), check_vma=False
    )
```

```python
import functools

import jax
import jax.numpy as jnp
from jax import lax
from jax.experimental import pallas as pl
from jax.experimental.pallas import tpu as pltpu
from jax.sharding import PartitionSpec as P

BLOCK = 512
EDGES = (0, 128, 256, 384, 512)
MESH = pl.DeviceIdType.MESH
NT = (((1,), (1,)), ((), ()))


def slot_table(owner_slot, group_id, positions, per_group):
    blocks = owner_slot.shape[0]
    block_row = jnp.arange(blocks, dtype=jnp.int32)[:, None]
    block_col = jnp.arange(blocks, dtype=jnp.int32)[None, :]
    inside = (block_row // per_group == group_id) & (block_col <= block_row)
    wanted = jnp.arange(positions, dtype=jnp.int32)[:, None, None]
    matched = inside[None] & (owner_slot[None] == wanted)
    is_live = jnp.any(matched, axis=(1, 2))
    left_block = jnp.sum(jnp.where(matched, block_row[None], 0), axis=(1, 2))
    right_block = jnp.sum(jnp.where(matched, block_col[None], 0), axis=(1, 2))
    return (left_block, right_block, is_live)


STAGES = len(EDGES) - 1
PIECES = []
for stage in range(STAGES):
    PIECES.append((stage, EDGES[stage], EDGES[stage + 1], 0, EDGES[stage + 1]))
    if stage:
        PIECES.append((stage, 0, EDGES[stage], EDGES[stage], EDGES[stage + 1]))


def kernel(rows_n, cols_n, per_group, slots, table, panel, out, *scratch):
    count = len(PIECES)
    scratch = list(scratch)

    def take(number):
        taken = scratch[:number]
        del scratch[:number]
        return taken

    held = take(STAGES)
    ysend, yrecv, zsend, zrecv = take(count), take(count), take(count), take(count)
    right_hi, right_lo, local_sem, load_recv, load_send, y_send, y_recv, z_send, z_recv = scratch
    row, col = lax.axis_index("row"), lax.axis_index("col")
    chips = rows_n // 2
    far = cols_n // 4
    x, core = row // 2, row % 2
    h, low, y = col // 4, (col // 2) % 2, col % 2
    sibling = (row + 1 - 2 * core, col)
    pair = (row, h * 4 + (1 - low) * 2 + y)
    across = (row, h * 4 + low * 2 + 1 - y)
    beside = [(((x + d) % chips) * 2 + core, col) for d in range(1, chips)]
    ahead = [(row, ((h + d) % far) * 4 + low * 2 + y) for d in range(1, far)]
    partners = [sibling, pair, across] + beside + ahead

    fetches = []
    for stage in range(STAGES):
        fetch = pltpu.make_async_copy(
            panel.at[:, pl.ds(EDGES[stage], EDGES[stage + 1] - EDGES[stage])],
            held[stage].at[pl.ds(row * per_group, per_group), low],
            local_sem.at[stage],
        )
        fetch.start()
        fetches.append(fetch)
    barrier = pltpu.get_barrier_semaphore()
    for device in partners:
        pl.semaphore_signal(barrier, inc=1, device_id=device, device_id_type=MESH)
    pl.semaphore_wait(barrier, len(partners))

    sent = []

    def push(stage, group, side, half, device):
        block = group * per_group + half
        copy = pltpu.make_async_remote_copy(
            src_ref=held[stage].at[block, side],
            dst_ref=held[stage].at[block, side],
            send_sem=load_send.at[len(sent)],
            recv_sem=load_recv.at[stage, block, side],
            device_id=device,
            device_id_type=MESH,
        )
        copy.start()
        sent.append(copy)

    def arrive(stage, group, side, half):
        block = group * per_group + half
        pltpu.make_async_remote_copy(
            src_ref=held[stage].at[block, side],
            dst_ref=held[stage].at[block, side],
            send_sem=load_send.at[0],
            recv_sem=load_recv.at[stage, block, side],
            device_id=sibling,
            device_id_type=MESH,
        ).wait_recv()

    cut = per_group // 2
    ups, downs = list(range(cut)), list(range(cut, per_group))
    others = [((x + chips - d) % chips) * 2 + core for d in range(1, chips)]

    def first(stage):
        fetches[stage].wait()
        for half in ups + downs:
            for device in beside:
                push(stage, row, low, half, device)
        for half in downs + ups:
            push(stage, row, low, half, pair)
        for half in ups + downs:
            push(stage, row, low, half, sibling)

    def second(stage):
        for group in others:
            for half in ups:
                arrive(stage, group, low, half)
                push(stage, group, low, half, pair)
                push(stage, group, low, half, sibling)
        for half in downs:
            arrive(stage, row, 1 - low, half)
            for device in beside:
                push(stage, row, 1 - low, half, device)
            push(stage, row, 1 - low, half, sibling)

    def third(stage):
        for group in others:
            for half in downs:
                arrive(stage, group, low, half)
                push(stage, group, low, half, sibling)
        for half in ups:
            arrive(stage, row, 1 - low, half)
            push(stage, row, 1 - low, half, sibling)
        for group in others:
            for half in ups + downs:
                arrive(stage, group, 1 - low, half)
                push(stage, group, 1 - low, half, sibling)
        for d in range(chips):
            group = ((x + d) % chips) * 2 + 1 - core
            for side in range(2):
                for half in range(per_group):
                    arrive(stage, group, side, half)

    depth = held[0].shape[-1]

    def split(value):
        top = value.astype(jnp.bfloat16)
        return top, (value - top.astype(jnp.float32)).astype(jnp.bfloat16)

    def strips(stage, position, emit, fresh=0):
        left, right = table[0, position], table[1, position]
        for part in range(fresh, stage + 1):
            for side in range(2):
                where = (slice(EDGES[part], EDGES[part + 1]), slice(side * depth, (side + 1) * depth))
                right_hi[where], right_lo[where] = split(held[part][right, side])

        def product(part, begin, end):
            total = None
            for side in range(2):
                span = slice(side * depth, (side + 1) * depth)
                top, rest = split(held[part][left, side])
                for one, two in ((rest, right_hi), (top, right_lo), (top, right_hi)):
                    term = lax.dot_general(one, two[begin:end, span], NT, preferred_element_type=jnp.float32)
                    total = term if total is None else total + term
            return total

        for number, (own_stage, r0, r1, c0, c1) in enumerate(PIECES):
            if own_stage == stage:
                for part in range(STAGES):
                    if r0 <= EDGES[part] < r1:
                        emit(number, EDGES[part] - r0, EDGES[part + 1] - r0, product(part, c0, c1))

    def numbers(stage):
        return [number for number, piece in enumerate(PIECES) if piece[0] == stage]

    def place(d, side_y, slot):
        return (((h + d) % far) * 4 + low * 2 + side_y) * slots + slot

    def y_copy(number, index):
        return pltpu.make_async_remote_copy(
            src_ref=ysend[number].at[index],
            dst_ref=yrecv[number].at[index],
            send_sem=y_send.at[number, index],
            recv_sem=y_recv.at[number, index],
            device_id=across,
            device_id_type=MESH,
        )

    def z_copy(number, index):
        return pltpu.make_async_remote_copy(
            src_ref=zsend[number].at[index],
            dst_ref=zrecv[number].at[index],
            send_sem=z_send.at[number, index],
            recv_sem=z_recv.at[number, index],
            device_id=(row, ((h + index // slots + 1) % far) * 4 + low * 2 + y),
            device_id_type=MESH,
        )

    tiles, hops = far * slots, (far - 1) * slots

    def y_work(stage):
        @pl.loop(0, tiles)
        def _(index):
            def emit(number, begin, end, value):
                ysend[number][index, begin:end, :] = value

            strips(stage, place(index // slots + 1, 1 - y, index % slots), emit)
            for number in numbers(stage):
                y_copy(number, index).start()

    def z_work(stage):
        @pl.loop(0, hops)
        def _(index):
            def emit(number, begin, end, value):
                zsend[number][index, begin:end, :] = value

            strips(stage, place(index // slots + 1, y, index % slots), emit)
            for number in numbers(stage):
                y_copy(number, index).wait_recv()
                zsend[number][index] += yrecv[number][index]
                z_copy(number, index).start()

    first(0)
    for stage in range(STAGES):
        second(stage)
        if stage + 1 < STAGES:
            first(stage + 1)
        if stage:
            z_work(stage - 1)
        third(stage)
        y_work(stage)
    z_work(STAGES - 1)

    @pl.loop(0, slots)
    def _(slot):
        def emit(number, begin, end, value):
            _, r0, _, c0, c1 = PIECES[number]
            out[slot, r0 + begin:r0 + end, c0:c1] = value

        for stage in range(STAGES):
            strips(stage, place(0, y, slot), emit, stage)
        for number, (_, r0, r1, c0, c1) in enumerate(PIECES):
            y_copy(number, hops + slot).wait_recv()
            out[slot, r0:r1, c0:c1] += yrecv[number][hops + slot]

    for number, (_, r0, r1, c0, c1) in enumerate(PIECES):
        @pl.loop(0, hops)
        def _(index):
            z_copy(number, index).wait_recv()
            slot = index % slots
            out[slot, r0:r1, c0:c1] += zrecv[number][index]

    for slot in range(slots):
        live = table[2, place(0, y, slot)]
        out[slot] = jnp.where(live > 0, out[slot], 0.0)

    for copy in sent:
        copy.wait_send()
    for number in range(count):
        @pl.loop(0, tiles)
        def _(index):
            y_copy(number, index).wait_send()

        @pl.loop(0, hops)
        def _(index):
            z_copy(number, index).wait_send()


def general(panel_rows, owner_slot):
    rows_n = lax.axis_size("row")
    cols_n = lax.axis_size("col")
    slab_rows, depth = panel_rows.shape
    per_group = slab_rows // BLOCK
    blocks = per_group * rows_n
    row_tiles = per_group * (blocks - per_group) + per_group * (per_group + 1) // 2
    slots = (row_tiles + cols_n - 1) // cols_n
    positions = cols_n * slots
    table = jnp.stack([part.astype(jnp.int32) for part in slot_table(owner_slot, lax.axis_index("row"), positions, per_group)])
    chips, far = rows_n // 2, cols_n // 4
    pushes = per_group * ((chips - 1) * 4 + 3) + per_group * (chips - 1)
    tiles = far * slots
    hops = (far - 1) * slots
    summed = pl.pallas_call(
        functools.partial(kernel, rows_n, cols_n, per_group, slots),
        out_shape=jax.ShapeDtypeStruct((slots, BLOCK, BLOCK), jnp.float32),
        in_specs=[pl.BlockSpec(memory_space=pltpu.SMEM), pl.BlockSpec(memory_space=pl.ANY)],
        out_specs=pl.BlockSpec(memory_space=pltpu.VMEM),
        scratch_shapes=[pltpu.VMEM((blocks, 2, EDGES[stage + 1] - EDGES[stage], depth), jnp.float32) for stage in range(STAGES)]
        + [
            pltpu.VMEM((number, r1 - r0, c1 - c0), jnp.float32)
            for number in (tiles, tiles, hops, hops)
            for _, r0, r1, c0, c1 in PIECES
        ]
        + [
            pltpu.VMEM((BLOCK, 2 * depth), jnp.bfloat16),
            pltpu.VMEM((BLOCK, 2 * depth), jnp.bfloat16),
            pltpu.SemaphoreType.DMA((STAGES,)),
            pltpu.SemaphoreType.DMA((STAGES, blocks, 2)),
            pltpu.SemaphoreType.DMA((STAGES * pushes,)),
            pltpu.SemaphoreType.DMA((len(PIECES), tiles)),
            pltpu.SemaphoreType.DMA((len(PIECES), tiles)),
            pltpu.SemaphoreType.DMA((len(PIECES), hops)),
            pltpu.SemaphoreType.DMA((len(PIECES), hops)),
        ],
        compiler_params=pltpu.CompilerParams(
            collective_id=0, has_side_effects=True, vmem_limit_bytes=60 * 2**20
        ),
        cost_estimate=pl.CostEstimate(flops=2 * positions * BLOCK * BLOCK * depth, bytes_accessed=2**22, transcendentals=0),
    )(table, panel_rows.reshape(per_group, BLOCK, depth))
    return summed[None]


LANES = 128
TALL = (0, 64, 128, 192, 256, 320, 384, 448, 512)
REACH = (128, 256, 384, 512, 512, 512, 512, 512)
STEP = 64
STEPS = BLOCK // STEP
AREAS = ((3, 0, 128), (3, 128, 256), (5, 256, 384), (7, 384, 512))
FULL = REACH.index(BLOCK)
FAST_STAGES = len(REACH)
FIRST = 4
PLAN = ((0, 0), (1, 0), (2, 0), (4, 4), (4, 5), (0, 1), (1, 1), (4, 6), (2, 1), (4, 7), (0, 2), (1, 2), (2, 2), (0, 3), (5, 6), (0, 4), (5, 7), (1, 3), (2, 4), (0, 5), (1, 4), (3, 3), (0, 6), (2, 5), (1, 5), (3, 5), (0, 7), (2, 6), (1, 6), (1, 7), (2, 7), (3, 7))
FAR, ACROSS, PASS, OWN = range(4)


def fast_pieces():
    pieces, before = [], 0
    for stage, reach in enumerate(REACH):
        pieces.append((stage, TALL[stage], TALL[stage + 1], 0, reach))
        if stage and reach > before:
            pieces.append((stage, 0, TALL[stage], before, reach))
        before = reach
    return pieces


FAST_PIECES = fast_pieces()


def fast_kernel(slots, source, panel, out, *scratch):
    count = len(FAST_PIECES)
    scratch = list(scratch)

    def take(number):
        taken = scratch[:number]
        del scratch[:number]
        return taken

    ysend, yrecv, zsend, zrecv = take(count), take(count), take(count), take(count)
    held, high, rest, total, table, owner, owner_sem, local_sem, load_recv, cross_recv, load_send, y_send, f_recv, o_recv, z_send, z_recv = scratch
    per_group = panel.shape[0]
    depth = panel.shape[-1]
    row, col = lax.axis_index("row"), lax.axis_index("col")
    x, core = row // 2, row % 2
    h, low, y = col // 4, (col // 2) % 2, col % 2
    sibling = (row + 1 - 2 * core, col)
    pair = (row, h * 4 + (1 - low) * 2 + y)
    across = (row, h * 4 + low * 2 + 1 - y)
    opposite = (row, (1 - h) * 4 + (1 - low) * 2 + y)
    beside = ((1 - x) * 2 + core, col)
    partners = [sibling, pair, across, opposite, beside]
    halves = range(per_group)

    barrier = pltpu.get_barrier_semaphore()
    for device in partners:
        pl.semaphore_signal(barrier, inc=1, device_id=device, device_id_type=MESH)
    fetches = []
    for step in range(STEPS):
        fetch = pltpu.make_async_copy(
            panel.at[:, pl.ds(step * STEP, STEP)],
            held.at[pl.ds(row * per_group, per_group), low, pl.ds(step * STEP, STEP)],
            local_sem.at[step],
        )
        fetch.start()
        fetches.append(fetch)
    notice = pltpu.make_async_copy(source, owner, owner_sem)
    notice.start()
    pl.semaphore_wait(barrier, len(partners))

    def load_copy(arrivals, step, group, side, device, kind):
        rows = pl.ds(0, BLOCK) if step is None else pl.ds(step * STEP, STEP)
        where = held.at[pl.ds(group * per_group, per_group), side, rows]
        return pltpu.make_async_remote_copy(
            src_ref=where,
            dst_ref=where,
            send_sem=load_send.at[kind],
            recv_sem=arrivals.at[0 if step is None else step, group % 2, side],
            device_id=device,
            device_id_type=MESH,
        )

    def push(arrivals, step, group, side, device, kind):
        load_copy(arrivals, step, group, side, device, kind).start()

    def arrive(arrivals, step, group, side):
        load_copy(arrivals, step, group, side, sibling, 0).wait_recv()

    other, flip = x * 2 + 1 - core, 1 - low

    def forward(step, side, kind):
        @pl.when(x == 0)
        def _():
            push(cross_recv, step, row, side, beside, kind)

    def begin(step):
        fetches[step].wait()
        if step == 0:
            forward(0, low, 3)
        push(load_recv, step, row, low, pair, 0)
        push(load_recv, step, row, low, sibling, 1)

    def gather(stage):
        start = REACH[stage - 1] if stage else 0
        steps = range(start // STEP, REACH[stage] // STEP)
        parts = range(TALL[stage] // STEP, TALL[stage + 1] // STEP)
        for step in steps:
            arrive(load_recv, step, row, flip)
            forward(step, flip, 4)
            if step + 1 < STEPS:
                forward(step + 1, low, 3)
            push(load_recv, step, row, flip, sibling, 2)

        @pl.when(x == 1)
        def _():
            for part in parts:
                for kind, side in ((5, low), (6, flip)):
                    arrive(cross_recv, part, core, side)
                    push(cross_recv, part, core, side, sibling, kind)

        for step in steps:
            for side in range(2):
                arrive(load_recv, step, other, side)

        @pl.when(x == 1)
        def _():
            for part in parts:
                for side in range(2):
                    arrive(cross_recv, part, 1 - core, side)

    def split(block, begin_row, end_row):
        for side in range(2):
            value = held[block, side, begin_row:end_row, :]
            top = value.astype(jnp.bfloat16)
            span = slice(side * depth, (side + 1) * depth)
            high[block, begin_row:end_row, span] = top
            rest[block, begin_row:end_row, span] = (value - top.astype(jnp.float32)).astype(jnp.bfloat16)

    def convert(stage):
        start = REACH[stage - 1] if stage else 0

        @pl.loop(0, per_group)
        def _(half):
            if start < REACH[stage]:
                split(row * per_group + half, start, REACH[stage])
            split(other * per_group + half, TALL[stage], TALL[stage + 1])

        @pl.when(x == 1)
        def _():
            @pl.loop(0, 2 * per_group)
            def _(block):
                split(block, TALL[stage], TALL[stage + 1])

    def numbers(stage):
        return [number for number, piece in enumerate(FAST_PIECES) if piece[0] == stage]

    def product(area, entry):
        r0, r1, c0, c1 = area
        wide, tall = table[0, entry], table[1, entry]
        top, low_part = high[tall, r0:r1, :], rest[tall, r0:r1, :]
        both = lax.dot_general(
            jnp.concatenate([top, low_part], axis=0), high[wide, c0:c1, :], NT, preferred_element_type=jnp.float32
        )
        cross = lax.dot_general(top, rest[wide, c0:c1, :], NT, preferred_element_type=jnp.float32)
        return both[r1 - r0:] + cross + both[:r1 - r0]

    def y_copy(number, kind, index):
        return pltpu.make_async_remote_copy(
            src_ref=ysend[number].at[index],
            dst_ref=yrecv[number].at[index],
            send_sem=y_send,
            recv_sem=(f_recv.at[number, index] if kind == FAR else o_recv.at[number]),
            device_id=across,
            device_id_type=MESH,
        )

    def z_copy(number, index):
        return pltpu.make_async_remote_copy(
            src_ref=zsend[number].at[index],
            dst_ref=zrecv[number].at[index],
            send_sem=z_send,
            recv_sem=z_recv.at[number],
            device_id=opposite,
            device_id_type=MESH,
        )

    def y_work(stage, kind):
        @pl.loop(0, slots)
        def _(slot):
            index = kind * slots + slot
            for number in numbers(stage):
                ysend[number][index] = product(FAST_PIECES[number][1:], index)
                y_copy(number, kind, index).start()

    def z_part(stage, slot):
        for number in numbers(stage):
            value = product(FAST_PIECES[number][1:], PASS * slots + slot)
            y_copy(number, FAR, FAR * slots + slot).wait_recv()
            zsend[number][slot] = value + yrecv[number][FAR * slots + slot]
            z_copy(number, slot).start()

    def z_work(stage):
        @pl.loop(0, slots)
        def _(slot):
            z_part(stage, slot)

    def z_half(entry):
        z_part(entry // slots, entry % slots)

    def own_work(stage):
        @pl.loop(0, slots)
        def _(slot):
            for last, r0, r1 in AREAS:
                if last == stage:
                    total[slot, r0:r1, :] = product((r0, r1, 0, BLOCK), OWN * slots + slot)

    def collect(stage):
        for number in numbers(stage):
            _, r0, r1, c0, c1 = FAST_PIECES[number]
            y_copy(number, ACROSS, pl.ds(ACROSS * slots, slots)).wait_recv()
            z_copy(number, pl.ds(0, slots)).wait_recv()

            @pl.loop(0, slots)
            def _(slot):
                total[slot, r0:r1, c0:c1] += yrecv[number][ACROSS * slots + slot] + zrecv[number][slot]

    def finish(part):
        for slot in range(slots):
            live = table[2, OWN * slots + slot]
            for c0 in range(0, BLOCK, LANES):
                value = total[slot, part * LANES:(part + 1) * LANES, c0:c0 + LANES].T
                out[slot, c0:c0 + LANES, part * LANES:(part + 1) * LANES] = jnp.where(live > 0, value, 0.0)

    for step in range(FIRST):
        begin(step)
    notice.wait()
    for kind, place in (
        (FAR, (1 - h) * 4 + (1 - low) * 2 + 1 - y),
        (ACROSS, h * 4 + low * 2 + 1 - y),
        (PASS, (1 - h) * 4 + (1 - low) * 2 + y),
        (OWN, h * 4 + low * 2 + y),
    ):
        for slot in range(slots):
            position = place * slots + slot
            left, right, live = row * per_group, row * per_group, 0
            for half in halves:
                for block in range(owner.shape[1]):
                    hit = owner[row * per_group + half, block] == position
                    left = jnp.where(hit, row * per_group + half, left)
                    right = jnp.where(hit, block, right)
                    live = jnp.where(hit, 1, live)
            table[0, kind * slots + slot] = left
            table[1, kind * slots + slot] = right
            table[2, kind * slots + slot] = live

    def supply(stage):
        gather(stage)
        convert(stage)
        y_work(stage, FAR)

    def relay(stage):
        y_work(stage, ACROSS)

    acts = (supply, relay, z_work, own_work, begin, z_half)
    for act, argument in PLAN:
        acts[act](argument)
    ready = 0
    for stage in range(FAST_STAGES):
        collect(stage)
        while stage >= FULL and (ready + 1) * LANES <= TALL[stage + 1]:
            finish(ready)
            ready += 1

    for side, kind in ((low, 0), (low, 1), (flip, 2)):
        load_copy(load_recv, None, row, side, sibling, kind).wait_send()

    @pl.when(x == 0)
    def _():
        for side, kind in ((low, 3), (flip, 4)):
            load_copy(cross_recv, None, row, side, sibling, kind).wait_send()

    @pl.when(x == 1)
    def _():
        for side, kind in ((low, 5), (flip, 6)):
            load_copy(cross_recv, None, core, side, sibling, kind).wait_send()

    for area, sem in ((held.at[pl.ds(0, slots)], y_send), (held.at[pl.ds(0, slots), 0], z_send)):
        pltpu.make_async_remote_copy(
            src_ref=area, dst_ref=area, send_sem=sem, recv_sem=o_recv.at[0], device_id=across, device_id_type=MESH
        ).wait_send()


def quick(panel_rows, owner_slot):
    rows_n = lax.axis_size("row")
    cols_n = lax.axis_size("col")
    slab_rows, depth = panel_rows.shape
    per_group = slab_rows // BLOCK
    blocks = per_group * rows_n
    row_tiles = per_group * (blocks - per_group) + per_group * (per_group + 1) // 2
    slots = (row_tiles + cols_n - 1) // cols_n
    positions = cols_n * slots
    count = len(FAST_PIECES)
    summed = pl.pallas_call(
        functools.partial(fast_kernel, slots),
        out_shape=pltpu.VMEM((slots, BLOCK, BLOCK), jnp.float32),
        in_specs=[pl.BlockSpec(memory_space=pl.ANY), pl.BlockSpec(memory_space=pl.ANY)],
        out_specs=pl.BlockSpec(memory_space=pltpu.VMEM),
        scratch_shapes=[
            pltpu.VMEM((number, r1 - r0, c1 - c0), jnp.float32)
            for number in (2 * slots, 2 * slots, slots, slots)
            for _, r0, r1, c0, c1 in FAST_PIECES
        ]
        + [
            pltpu.VMEM((blocks, 2, BLOCK, depth), jnp.float32),
            pltpu.VMEM((blocks, BLOCK, 2 * depth), jnp.bfloat16),
            pltpu.VMEM((blocks, BLOCK, 2 * depth), jnp.bfloat16),
            pltpu.VMEM((slots, BLOCK, BLOCK), jnp.float32),
            pltpu.SMEM((3, 4 * slots), jnp.int32),
            pltpu.SMEM(owner_slot.shape, jnp.int32),
            pltpu.SemaphoreType.DMA(()),
            pltpu.SemaphoreType.DMA((STEPS,)),
            pltpu.SemaphoreType.DMA((STEPS, 2, 2)),
            pltpu.SemaphoreType.DMA((STEPS, 2, 2)),
            pltpu.SemaphoreType.DMA((7,)),
            pltpu.SemaphoreType.DMA(()),
            pltpu.SemaphoreType.DMA((count, slots)),
            pltpu.SemaphoreType.DMA((count,)),
            pltpu.SemaphoreType.DMA(()),
            pltpu.SemaphoreType.DMA((count,)),
        ],
        compiler_params=pltpu.CompilerParams(
            collective_id=0, has_side_effects=True, vmem_limit_bytes=54 * 2**20
        ),
        cost_estimate=pl.CostEstimate(flops=2 * positions * BLOCK * BLOCK * depth, bytes_accessed=2**22, transcendentals=0),
    )(owner_slot, panel_rows.reshape(per_group, BLOCK, depth))
    return summed[None]


def body(panel_rows, owner_slot):
    if lax.axis_size("row") == 4 and lax.axis_size("col") == 8:
        return quick(panel_rows, owner_slot)
    return general(panel_rows, owner_slot)


def solution(mesh):
    placed = (P("row", "col"), P())
    return jax.shard_map(
        body, mesh=mesh, in_specs=placed, out_specs=P("row", "col", None, None), check_vma=False
    )
```

```python
import functools

import jax
import jax.numpy as jnp
from jax import lax
from jax.experimental import pallas as pl
from jax.experimental.pallas import tpu as pltpu
from jax.sharding import PartitionSpec as P

BLOCK = 512
EDGES = (0, 128, 256, 384, 512)
MESH = pl.DeviceIdType.MESH
NT = (((1,), (1,)), ((), ()))


def slot_table(owner_slot, group_id, positions, per_group):
    blocks = owner_slot.shape[0]
    block_row = jnp.arange(blocks, dtype=jnp.int32)[:, None]
    block_col = jnp.arange(blocks, dtype=jnp.int32)[None, :]
    inside = (block_row // per_group == group_id) & (block_col <= block_row)
    wanted = jnp.arange(positions, dtype=jnp.int32)[:, None, None]
    matched = inside[None] & (owner_slot[None] == wanted)
    is_live = jnp.any(matched, axis=(1, 2))
    left_block = jnp.sum(jnp.where(matched, block_row[None], 0), axis=(1, 2))
    right_block = jnp.sum(jnp.where(matched, block_col[None], 0), axis=(1, 2))
    return (left_block, right_block, is_live)


STAGES = len(EDGES) - 1
PIECES = []
for stage in range(STAGES):
    PIECES.append((stage, EDGES[stage], EDGES[stage + 1], 0, EDGES[stage + 1]))
    if stage:
        PIECES.append((stage, 0, EDGES[stage], EDGES[stage], EDGES[stage + 1]))


def kernel(rows_n, cols_n, per_group, slots, table, panel, out, *scratch):
    count = len(PIECES)
    scratch = list(scratch)

    def take(number):
        taken = scratch[:number]
        del scratch[:number]
        return taken

    held = take(STAGES)
    ysend, yrecv, zsend, zrecv = take(count), take(count), take(count), take(count)
    right_hi, right_lo, local_sem, load_recv, load_send, y_send, y_recv, z_send, z_recv = scratch
    row, col = lax.axis_index("row"), lax.axis_index("col")
    chips = rows_n // 2
    far = cols_n // 4
    x, core = row // 2, row % 2
    h, low, y = col // 4, (col // 2) % 2, col % 2
    sibling = (row + 1 - 2 * core, col)
    pair = (row, h * 4 + (1 - low) * 2 + y)
    across = (row, h * 4 + low * 2 + 1 - y)
    beside = [(((x + d) % chips) * 2 + core, col) for d in range(1, chips)]
    ahead = [(row, ((h + d) % far) * 4 + low * 2 + y) for d in range(1, far)]
    partners = [sibling, pair, across] + beside + ahead

    fetches = []
    for stage in range(STAGES):
        fetch = pltpu.make_async_copy(
            panel.at[:, pl.ds(EDGES[stage], EDGES[stage + 1] - EDGES[stage])],
            held[stage].at[pl.ds(row * per_group, per_group), low],
            local_sem.at[stage],
        )
        fetch.start()
        fetches.append(fetch)
    barrier = pltpu.get_barrier_semaphore()
    for device in partners:
        pl.semaphore_signal(barrier, inc=1, device_id=device, device_id_type=MESH)
    pl.semaphore_wait(barrier, len(partners))

    sent = []

    def push(stage, group, side, half, device):
        block = group * per_group + half
        copy = pltpu.make_async_remote_copy(
            src_ref=held[stage].at[block, side],
            dst_ref=held[stage].at[block, side],
            send_sem=load_send.at[len(sent)],
            recv_sem=load_recv.at[stage, block, side],
            device_id=device,
            device_id_type=MESH,
        )
        copy.start()
        sent.append(copy)

    def arrive(stage, group, side, half):
        block = group * per_group + half
        pltpu.make_async_remote_copy(
            src_ref=held[stage].at[block, side],
            dst_ref=held[stage].at[block, side],
            send_sem=load_send.at[0],
            recv_sem=load_recv.at[stage, block, side],
            device_id=sibling,
            device_id_type=MESH,
        ).wait_recv()

    cut = per_group // 2
    ups, downs = list(range(cut)), list(range(cut, per_group))
    others = [((x + chips - d) % chips) * 2 + core for d in range(1, chips)]

    def first(stage):
        fetches[stage].wait()
        for half in ups + downs:
            for device in beside:
                push(stage, row, low, half, device)
        for half in downs + ups:
            push(stage, row, low, half, pair)
        for half in ups + downs:
            push(stage, row, low, half, sibling)

    def second(stage):
        for group in others:
            for half in ups:
                arrive(stage, group, low, half)
                push(stage, group, low, half, pair)
                push(stage, group, low, half, sibling)
        for half in downs:
            arrive(stage, row, 1 - low, half)
            for device in beside:
                push(stage, row, 1 - low, half, device)
            push(stage, row, 1 - low, half, sibling)

    def third(stage):
        for group in others:
            for half in downs:
                arrive(stage, group, low, half)
                push(stage, group, low, half, sibling)
        for half in ups:
            arrive(stage, row, 1 - low, half)
            push(stage, row, 1 - low, half, sibling)
        for group in others:
            for half in ups + downs:
                arrive(stage, group, 1 - low, half)
                push(stage, group, 1 - low, half, sibling)
        for d in range(chips):
            group = ((x + d) % chips) * 2 + 1 - core
            for side in range(2):
                for half in range(per_group):
                    arrive(stage, group, side, half)

    depth = held[0].shape[-1]

    def split(value):
        top = value.astype(jnp.bfloat16)
        return top, (value - top.astype(jnp.float32)).astype(jnp.bfloat16)

    def strips(stage, position, emit, fresh=0):
        left, right = table[0, position], table[1, position]
        for part in range(fresh, stage + 1):
            for side in range(2):
                where = (slice(EDGES[part], EDGES[part + 1]), slice(side * depth, (side + 1) * depth))
                right_hi[where], right_lo[where] = split(held[part][right, side])

        def product(part, begin, end):
            total = None
            for side in range(2):
                span = slice(side * depth, (side + 1) * depth)
                top, rest = split(held[part][left, side])
                for one, two in ((rest, right_hi), (top, right_lo), (top, right_hi)):
                    term = lax.dot_general(one, two[begin:end, span], NT, preferred_element_type=jnp.float32)
                    total = term if total is None else total + term
            return total

        for number, (own_stage, r0, r1, c0, c1) in enumerate(PIECES):
            if own_stage == stage:
                for part in range(STAGES):
                    if r0 <= EDGES[part] < r1:
                        emit(number, EDGES[part] - r0, EDGES[part + 1] - r0, product(part, c0, c1))

    def numbers(stage):
        return [number for number, piece in enumerate(PIECES) if piece[0] == stage]

    def place(d, side_y, slot):
        return (((h + d) % far) * 4 + low * 2 + side_y) * slots + slot

    def y_copy(number, index):
        return pltpu.make_async_remote_copy(
            src_ref=ysend[number].at[index],
            dst_ref=yrecv[number].at[index],
            send_sem=y_send.at[number, index],
            recv_sem=y_recv.at[number, index],
            device_id=across,
            device_id_type=MESH,
        )

    def z_copy(number, index):
        return pltpu.make_async_remote_copy(
            src_ref=zsend[number].at[index],
            dst_ref=zrecv[number].at[index],
            send_sem=z_send.at[number, index],
            recv_sem=z_recv.at[number, index],
            device_id=(row, ((h + index // slots + 1) % far) * 4 + low * 2 + y),
            device_id_type=MESH,
        )

    tiles, hops = far * slots, (far - 1) * slots

    def y_work(stage):
        @pl.loop(0, tiles)
        def _(index):
            def emit(number, begin, end, value):
                ysend[number][index, begin:end, :] = value

            strips(stage, place(index // slots + 1, 1 - y, index % slots), emit)
            for number in numbers(stage):
                y_copy(number, index).start()

    def z_work(stage):
        @pl.loop(0, hops)
        def _(index):
            def emit(number, begin, end, value):
                zsend[number][index, begin:end, :] = value

            strips(stage, place(index // slots + 1, y, index % slots), emit)
            for number in numbers(stage):
                y_copy(number, index).wait_recv()
                zsend[number][index] += yrecv[number][index]
                z_copy(number, index).start()

    first(0)
    for stage in range(STAGES):
        second(stage)
        if stage + 1 < STAGES:
            first(stage + 1)
        if stage:
            z_work(stage - 1)
        third(stage)
        y_work(stage)
    z_work(STAGES - 1)

    @pl.loop(0, slots)
    def _(slot):
        def emit(number, begin, end, value):
            _, r0, _, c0, c1 = PIECES[number]
            out[slot, r0 + begin:r0 + end, c0:c1] = value

        for stage in range(STAGES):
            strips(stage, place(0, y, slot), emit, stage)
        for number, (_, r0, r1, c0, c1) in enumerate(PIECES):
            y_copy(number, hops + slot).wait_recv()
            out[slot, r0:r1, c0:c1] += yrecv[number][hops + slot]

    for number, (_, r0, r1, c0, c1) in enumerate(PIECES):
        @pl.loop(0, hops)
        def _(index):
            z_copy(number, index).wait_recv()
            slot = index % slots
            out[slot, r0:r1, c0:c1] += zrecv[number][index]

    for slot in range(slots):
        live = table[2, place(0, y, slot)]
        out[slot] = jnp.where(live > 0, out[slot], 0.0)

    for copy in sent:
        copy.wait_send()
    for number in range(count):
        @pl.loop(0, tiles)
        def _(index):
            y_copy(number, index).wait_send()

        @pl.loop(0, hops)
        def _(index):
            z_copy(number, index).wait_send()


def general(panel_rows, owner_slot):
    rows_n = lax.axis_size("row")
    cols_n = lax.axis_size("col")
    slab_rows, depth = panel_rows.shape
    per_group = slab_rows // BLOCK
    blocks = per_group * rows_n
    row_tiles = per_group * (blocks - per_group) + per_group * (per_group + 1) // 2
    slots = (row_tiles + cols_n - 1) // cols_n
    positions = cols_n * slots
    table = jnp.stack([part.astype(jnp.int32) for part in slot_table(owner_slot, lax.axis_index("row"), positions, per_group)])
    chips, far = rows_n // 2, cols_n // 4
    pushes = per_group * ((chips - 1) * 4 + 3) + per_group * (chips - 1)
    tiles = far * slots
    hops = (far - 1) * slots
    summed = pl.pallas_call(
        functools.partial(kernel, rows_n, cols_n, per_group, slots),
        out_shape=jax.ShapeDtypeStruct((slots, BLOCK, BLOCK), jnp.float32),
        in_specs=[pl.BlockSpec(memory_space=pltpu.SMEM), pl.BlockSpec(memory_space=pl.ANY)],
        out_specs=pl.BlockSpec(memory_space=pltpu.VMEM),
        scratch_shapes=[pltpu.VMEM((blocks, 2, EDGES[stage + 1] - EDGES[stage], depth), jnp.float32) for stage in range(STAGES)]
        + [
            pltpu.VMEM((number, r1 - r0, c1 - c0), jnp.float32)
            for number in (tiles, tiles, hops, hops)
            for _, r0, r1, c0, c1 in PIECES
        ]
        + [
            pltpu.VMEM((BLOCK, 2 * depth), jnp.bfloat16),
            pltpu.VMEM((BLOCK, 2 * depth), jnp.bfloat16),
            pltpu.SemaphoreType.DMA((STAGES,)),
            pltpu.SemaphoreType.DMA((STAGES, blocks, 2)),
            pltpu.SemaphoreType.DMA((STAGES * pushes,)),
            pltpu.SemaphoreType.DMA((len(PIECES), tiles)),
            pltpu.SemaphoreType.DMA((len(PIECES), tiles)),
            pltpu.SemaphoreType.DMA((len(PIECES), hops)),
            pltpu.SemaphoreType.DMA((len(PIECES), hops)),
        ],
        compiler_params=pltpu.CompilerParams(
            collective_id=0, has_side_effects=True, vmem_limit_bytes=60 * 2**20
        ),
        cost_estimate=pl.CostEstimate(flops=2 * positions * BLOCK * BLOCK * depth, bytes_accessed=2**22, transcendentals=0),
    )(table, panel_rows.reshape(per_group, BLOCK, depth))
    return summed[None]


LANES = 128
TALL = (0, 64, 128, 192, 256, 320, 384, 448, 512)
REACH = (128, 256, 384, 512, 512, 512, 512, 512)
STEP = 64
STEPS = BLOCK // STEP
AREAS = ((3, 0, 128), (3, 128, 256), (5, 256, 384), (7, 384, 512))
FULL = REACH.index(BLOCK)
FAST_STAGES = len(REACH)
FIRST = 4
PLAN = ((0, 0), (1, 0), (2, 0), (4, 4), (4, 5), (0, 1), (1, 1), (4, 6), (2, 1), (4, 7), (0, 2), (1, 2), (2, 2), (0, 3), (5, 6), (0, 4), (5, 7), (1, 3), (2, 4), (0, 5), (1, 4), (0, 6), (2, 5), (1, 5), (3, 3), (0, 7), (2, 6), (1, 6), (1, 7), (3, 5), (2, 7), (3, 7))
FAR, ACROSS, PASS, OWN = range(4)


def fast_pieces():
    pieces, before = [], 0
    for stage, reach in enumerate(REACH):
        pieces.append((stage, TALL[stage], TALL[stage + 1], 0, reach))
        if stage and reach > before:
            pieces.append((stage, 0, TALL[stage], before, reach))
        before = reach
    return pieces


FAST_PIECES = fast_pieces()


def fast_kernel(slots, source, panel, out, *scratch):
    count = len(FAST_PIECES)
    scratch = list(scratch)

    def take(number):
        taken = scratch[:number]
        del scratch[:number]
        return taken

    ysend, yrecv, zsend, zrecv = take(count), take(count), take(count), take(count)
    held, high, rest, total, table, owner, owner_sem, local_sem, load_recv, cross_recv, load_send, y_send, f_recv, o_recv, z_send, z_recv = scratch
    per_group = panel.shape[0]
    depth = panel.shape[-1]
    row, col = lax.axis_index("row"), lax.axis_index("col")
    x, core = row // 2, row % 2
    h, low, y = col // 4, (col // 2) % 2, col % 2
    sibling = (row + 1 - 2 * core, col)
    pair = (row, h * 4 + (1 - low) * 2 + y)
    across = (row, h * 4 + low * 2 + 1 - y)
    opposite = (row, (1 - h) * 4 + (1 - low) * 2 + y)
    beside = ((1 - x) * 2 + core, col)
    partners = [sibling, pair, across, opposite, beside]
    halves = range(per_group)

    barrier = pltpu.get_barrier_semaphore()
    for device in partners:
        pl.semaphore_signal(barrier, inc=1, device_id=device, device_id_type=MESH)
    fetches = []
    for step in range(STEPS):
        fetch = pltpu.make_async_copy(
            panel.at[:, pl.ds(step * STEP, STEP)],
            held.at[pl.ds(row * per_group, per_group), low, pl.ds(step * STEP, STEP)],
            local_sem.at[step],
        )
        fetch.start()
        fetches.append(fetch)
    notice = pltpu.make_async_copy(source, owner, owner_sem)
    notice.start()
    pl.semaphore_wait(barrier, len(partners))

    def load_copy(arrivals, step, group, side, device, kind):
        rows = pl.ds(0, BLOCK) if step is None else pl.ds(step * STEP, STEP)
        where = held.at[pl.ds(group * per_group, per_group), side, rows]
        return pltpu.make_async_remote_copy(
            src_ref=where,
            dst_ref=where,
            send_sem=load_send.at[kind],
            recv_sem=arrivals.at[0 if step is None else step, group % 2, side],
            device_id=device,
            device_id_type=MESH,
        )

    def push(arrivals, step, group, side, device, kind):
        load_copy(arrivals, step, group, side, device, kind).start()

    def arrive(arrivals, step, group, side):
        load_copy(arrivals, step, group, side, sibling, 0).wait_recv()

    other, flip = x * 2 + 1 - core, 1 - low

    def forward(step, side, kind):
        @pl.when(x == 0)
        def _():
            push(cross_recv, step, row, side, beside, kind)

    def begin(step):
        fetches[step].wait()
        if step == 0:
            forward(0, low, 3)
        push(load_recv, step, row, low, pair, 0)
        push(load_recv, step, row, low, sibling, 1)

    def gather(stage):
        start = REACH[stage - 1] if stage else 0
        steps = range(start // STEP, REACH[stage] // STEP)
        parts = range(TALL[stage] // STEP, TALL[stage + 1] // STEP)
        for step in steps:
            arrive(load_recv, step, row, flip)
            forward(step, flip, 4)
            if step + 1 < STEPS:
                forward(step + 1, low, 3)
            push(load_recv, step, row, flip, sibling, 2)

        @pl.when(x == 1)
        def _():
            for part in parts:
                for kind, side in ((5, low), (6, flip)):
                    arrive(cross_recv, part, core, side)
                    push(cross_recv, part, core, side, sibling, kind)

        for step in steps:
            for side in range(2):
                arrive(load_recv, step, other, side)

        @pl.when(x == 1)
        def _():
            for part in parts:
                for side in range(2):
                    arrive(cross_recv, part, 1 - core, side)

    def split(block, begin_row, end_row):
        for side in range(2):
            value = held[block, side, begin_row:end_row, :]
            top = value.astype(jnp.bfloat16)
            span = slice(side * depth, (side + 1) * depth)
            high[block, begin_row:end_row, span] = top
            rest[block, begin_row:end_row, span] = (value - top.astype(jnp.float32)).astype(jnp.bfloat16)

    def convert(stage):
        start = REACH[stage - 1] if stage else 0

        @pl.loop(0, per_group)
        def _(half):
            if start < REACH[stage]:
                split(row * per_group + half, start, REACH[stage])
            split(other * per_group + half, TALL[stage], TALL[stage + 1])

        @pl.when(x == 1)
        def _():
            @pl.loop(0, 2 * per_group)
            def _(block):
                split(block, TALL[stage], TALL[stage + 1])

    def numbers(stage):
        return [number for number, piece in enumerate(FAST_PIECES) if piece[0] == stage]

    def product(area, entry):
        r0, r1, c0, c1 = area
        wide, tall = table[0, entry], table[1, entry]
        top, low_part = high[tall, r0:r1, :], rest[tall, r0:r1, :]
        both = lax.dot_general(
            jnp.concatenate([top, low_part], axis=0), high[wide, c0:c1, :], NT, preferred_element_type=jnp.float32
        )
        cross = lax.dot_general(top, rest[wide, c0:c1, :], NT, preferred_element_type=jnp.float32)
        return both[r1 - r0:] + cross + both[:r1 - r0]

    def y_copy(number, kind, index):
        return pltpu.make_async_remote_copy(
            src_ref=ysend[number].at[index],
            dst_ref=yrecv[number].at[index],
            send_sem=y_send,
            recv_sem=(f_recv.at[number, index] if kind == FAR else o_recv),
            device_id=across,
            device_id_type=MESH,
        )

    def z_copy(number, index):
        return pltpu.make_async_remote_copy(
            src_ref=zsend[number].at[index],
            dst_ref=zrecv[number].at[index],
            send_sem=z_send,
            recv_sem=z_recv.at[number],
            device_id=opposite,
            device_id_type=MESH,
        )

    def y_work(stage, kind):
        @pl.loop(0, slots)
        def _(slot):
            index = kind * slots + slot
            for number in numbers(stage):
                ysend[number][index] = product(FAST_PIECES[number][1:], index)
                y_copy(number, kind, index).start()

    def z_part(stage, slot):
        for number in numbers(stage):
            value = product(FAST_PIECES[number][1:], PASS * slots + slot)
            y_copy(number, FAR, FAR * slots + slot).wait_recv()
            zsend[number][slot] = value + yrecv[number][FAR * slots + slot]
            z_copy(number, slot).start()

    def z_work(stage):
        @pl.loop(0, slots)
        def _(slot):
            z_part(stage, slot)

    def z_half(entry):
        z_part(entry // slots, entry % slots)

    def own_work(stage):
        @pl.loop(0, slots)
        def _(slot):
            for last, r0, r1 in AREAS:
                if last == stage:
                    total[slot, r0:r1, :] = product((r0, r1, 0, BLOCK), OWN * slots + slot)

    def collect(stage):
        for number in numbers(stage):
            _, r0, r1, c0, c1 = FAST_PIECES[number]
            z_copy(number, pl.ds(0, slots)).wait_recv()

            @pl.loop(0, slots)
            def _(slot):
                total[slot, r0:r1, c0:c1] += yrecv[number][ACROSS * slots + slot] + zrecv[number][slot]

    def finish(part):
        for slot in range(slots):
            live = table[2, OWN * slots + slot]
            for c0 in range(0, BLOCK, LANES):
                value = total[slot, part * LANES:(part + 1) * LANES, c0:c0 + LANES].T
                out[slot, c0:c0 + LANES, part * LANES:(part + 1) * LANES] = jnp.where(live > 0, value, 0.0)

    for step in range(FIRST):
        begin(step)
    notice.wait()
    for kind, place in (
        (FAR, (1 - h) * 4 + (1 - low) * 2 + 1 - y),
        (ACROSS, h * 4 + low * 2 + 1 - y),
        (PASS, (1 - h) * 4 + (1 - low) * 2 + y),
        (OWN, h * 4 + low * 2 + y),
    ):
        for slot in range(slots):
            position = place * slots + slot
            left, right, live = row * per_group, row * per_group, 0
            for half in halves:
                for block in range(owner.shape[1]):
                    hit = owner[row * per_group + half, block] == position
                    left = jnp.where(hit, row * per_group + half, left)
                    right = jnp.where(hit, block, right)
                    live = jnp.where(hit, 1, live)
            table[0, kind * slots + slot] = left
            table[1, kind * slots + slot] = right
            table[2, kind * slots + slot] = live

    def supply(stage):
        gather(stage)
        convert(stage)
        y_work(stage, FAR)

    def relay(stage):
        y_work(stage, ACROSS)

    acts = (supply, relay, z_work, own_work, begin, z_half)
    for act, argument in PLAN:
        acts[act](argument)
    whole = held.at[pl.ds(0, slots), 0]
    pltpu.make_async_remote_copy(
        src_ref=whole, dst_ref=whole, send_sem=y_send, recv_sem=o_recv, device_id=across, device_id_type=MESH
    ).wait_recv()
    ready = 0
    for stage in range(FAST_STAGES):
        collect(stage)
        while stage >= FULL and (ready + 1) * LANES <= TALL[stage + 1]:
            finish(ready)
            ready += 1

    for side, kind in ((low, 0), (low, 1), (flip, 2)):
        load_copy(load_recv, None, row, side, sibling, kind).wait_send()

    @pl.when(x == 0)
    def _():
        for side, kind in ((low, 3), (flip, 4)):
            load_copy(cross_recv, None, row, side, sibling, kind).wait_send()

    @pl.when(x == 1)
    def _():
        for side, kind in ((low, 5), (flip, 6)):
            load_copy(cross_recv, None, core, side, sibling, kind).wait_send()

    for area, sem in ((held.at[pl.ds(0, slots)], y_send), (held.at[pl.ds(0, slots), 0], z_send)):
        pltpu.make_async_remote_copy(
            src_ref=area, dst_ref=area, send_sem=sem, recv_sem=o_recv, device_id=across, device_id_type=MESH
        ).wait_send()


def quick(panel_rows, owner_slot):
    rows_n = lax.axis_size("row")
    cols_n = lax.axis_size("col")
    slab_rows, depth = panel_rows.shape
    per_group = slab_rows // BLOCK
    blocks = per_group * rows_n
    row_tiles = per_group * (blocks - per_group) + per_group * (per_group + 1) // 2
    slots = (row_tiles + cols_n - 1) // cols_n
    positions = cols_n * slots
    count = len(FAST_PIECES)
    summed = pl.pallas_call(
        functools.partial(fast_kernel, slots),
        out_shape=pltpu.VMEM((slots, BLOCK, BLOCK), jnp.float32),
        in_specs=[pl.BlockSpec(memory_space=pl.ANY), pl.BlockSpec(memory_space=pl.ANY)],
        out_specs=pl.BlockSpec(memory_space=pltpu.VMEM),
        scratch_shapes=[
            pltpu.VMEM((number, r1 - r0, c1 - c0), jnp.float32)
            for number in (2 * slots, 2 * slots, slots, slots)
            for _, r0, r1, c0, c1 in FAST_PIECES
        ]
        + [
            pltpu.VMEM((blocks, 2, BLOCK, depth), jnp.float32),
            pltpu.VMEM((blocks, BLOCK, 2 * depth), jnp.bfloat16),
            pltpu.VMEM((blocks, BLOCK, 2 * depth), jnp.bfloat16),
            pltpu.VMEM((slots, BLOCK, BLOCK), jnp.float32),
            pltpu.SMEM((3, 4 * slots), jnp.int32),
            pltpu.SMEM(owner_slot.shape, jnp.int32),
            pltpu.SemaphoreType.DMA(()),
            pltpu.SemaphoreType.DMA((STEPS,)),
            pltpu.SemaphoreType.DMA((STEPS, 2, 2)),
            pltpu.SemaphoreType.DMA((STEPS, 2, 2)),
            pltpu.SemaphoreType.DMA((7,)),
            pltpu.SemaphoreType.DMA(()),
            pltpu.SemaphoreType.DMA((count, slots)),
            pltpu.SemaphoreType.DMA(()),
            pltpu.SemaphoreType.DMA(()),
            pltpu.SemaphoreType.DMA((count,)),
        ],
        compiler_params=pltpu.CompilerParams(
            collective_id=0, has_side_effects=True, vmem_limit_bytes=54 * 2**20
        ),
        cost_estimate=pl.CostEstimate(flops=2 * positions * BLOCK * BLOCK * depth, bytes_accessed=2**22, transcendentals=0),
    )(owner_slot, panel_rows.reshape(per_group, BLOCK, depth))
    return summed[None]


def body(panel_rows, owner_slot):
    if lax.axis_size("row") == 4 and lax.axis_size("col") == 8:
        return quick(panel_rows, owner_slot)
    return general(panel_rows, owner_slot)


def solution(mesh):
    placed = (P("row", "col"), P())
    return jax.shard_map(
        body, mesh=mesh, in_specs=placed, out_specs=P("row", "col", None, None), check_vma=False
    )
```
